32 devices in a mesh: groups: 2 (over x), tile: 16 (over z, y, core).
Axes of the slice: x: 2, y: 2, z: 4, core: 2. Of those that a mesh axis runs over, the one named last changes fastest.
Arguments:
- tracer_state: float32 [2, 50, 4096], P(None, None, ('groups', 'tile')), parts along dimension 2, may hold values from -6 to 6
- krylov_direction: float32 [2, 50, 4096], P(None, None, ('groups', 'tile')), parts along dimension 2, may hold values from -6 to 6
- explicit_tiles: bfloat16 [800, 6, 128, 128], P('tile')
- implicit_tiles: bfloat16 [800, 3, 128, 128], P('tile')
- explicit_columns: int32 [800, 6], P('tile'), may hold values from 0 to 450, as said below
- ghost_levels: int32 [256, 25], P('tile'), may hold values from 0 to 50, as said below
- wet_levels: int32 [2048], P('tile'), may hold values from 0 to 50
- surface_light: float32 [4096], P(('groups', 'tile')), parts along dimension 0, may hold values from 0.25 to 4
- martin_exponent: float32 [4096], P(('groups', 'tile')), parts along dimension 0, may hold values from 0.5 to 2
- column_slots: int32 [256, 12], P('tile'), may hold values from 0 to 128, as said below
Outputs:
- state_out: float32 [2, 50, 4096], P(None, None, ('groups', 'tile')), parts along dimension 2
- tangent_out: float32 [2, 50, 4096], P(None, None, ('groups', 'tile')), parts along dimension 2
- export_flux: float32 [6144], P(('groups', 'tile')), parts along dimension 0
The draws below stay inside these ranges and needn't reach their ends.
There are 2 independent parts, one for each index of `groups`. The reference program is written for one: setup_inputs(seed, part) draws one part's arguments, and reference() takes and returns one part's arrays. A program takes and returns all parts, laid end to end along the dimension named above; an argument that names none is the same for every part. Nothing has to cross between parts.
Inputs may be any that keep to these rules, and one draw needn't show every extreme that they name: `explicit_columns`: row d * 50 + l holds l, then l - 1 and l + 1 (50 beyond the ends), then one position for each of the devices d - 1, d + 1 and d + D / 2 of the D devices (wrapping), in that order: 51 + s * 25 + l when ghost_levels sends level l from that device s to d, else 50. `ghost_levels`: row s * D + d, slot k, holds k or 50. It holds k exactly for k below a depth of 1 to 25 when s is d - 1, d + 1 or d + D / 2 (wrapping), and 50 for all other pairs; some device gets depth 25 from all three. `column_slots`: row s * D + b lists local columns of device s handed to device b, 128 marking an empty slot. Each column of s with wet_levels above 0 stands exactly once in rows s * D to s * D + D - 1, no dry column does, and some row is full.
All inputs are finite; a program needn't handle non-finite values.
Results may differ from the reference program's by a relative error of at most 0.012.
Values may be sent and summed in bfloat16 or wider, within the bound.
No kernel may reach another device: no remote copies, remote signals or barrier semaphores. Data moves between devices by JAX's collectives and lax.ppermute only.
A program may use at most 64 MiB of HBM per device.

```python
import math
import jax
import jax.numpy as jnp
from jax import lax

LEVELS = 50
TRACERS = 2
DEVICE_COLUMNS = 128
NEIGHBOURS = 6
EUPHOTIC = 6
STEPS = 3
GHOST_DEPTH = 25
SLOTS = 12
COLUMNS = 2048
N_TILE = 16


def neighbour_offsets():
    device_count = COLUMNS // DEVICE_COLUMNS
    return jnp.array([1, -1, device_count // 2], dtype=jnp.int32)


def ghost_depths(key):
    device_count = COLUMNS // DEVICE_COLUMNS
    base_key = jax.random.fold_in(key, 11)
    shared_depth = jax.random.randint(base_key, (device_count, 3), 1, GHOST_DEPTH + 1)
    full_receiver = jax.random.randint(jax.random.fold_in(base_key, 1), (), 0, device_count)
    receivers = jnp.arange(device_count, dtype=jnp.int32)[:, None]
    return jnp.where(receivers == full_receiver, GHOST_DEPTH, shared_depth).astype(jnp.int32)


def draw_ghost_levels(key, part):
    device_count = COLUMNS // DEVICE_COLUMNS
    shared_depth = ghost_depths(key)
    receiver = jnp.arange(device_count, dtype=jnp.int32)[None, :, None]
    sender = jnp.arange(device_count, dtype=jnp.int32)[:, None, None]
    matches = (receiver - neighbour_offsets()[None, None, :]) % device_count == sender
    depth_limit = jnp.sum(jnp.where(matches, shared_depth[None, :, :], 0), -1)
    ghost_slot = jnp.arange(GHOST_DEPTH, dtype=jnp.int32)
    levels_sent = jnp.where(ghost_slot[None, None, :] < depth_limit[:, :, None], ghost_slot[None, None, :], LEVELS)
    return levels_sent.reshape(device_count * device_count, GHOST_DEPTH).astype(jnp.int32)


def draw_explicit_columns(key, part):
    device_count = COLUMNS // DEVICE_COLUMNS
    shared_depth = ghost_depths(key)
    level_index = jnp.arange(LEVELS, dtype=jnp.int32)
    index_of_device = jnp.arange(device_count, dtype=jnp.int32)
    own_level = jnp.broadcast_to(level_index[None, :, None], (device_count, LEVELS, 1))
    upper_level = jnp.broadcast_to(jnp.where(level_index >= 1, level_index - 1, LEVELS)[None, :, None], (device_count, LEVELS, 1))
    lower_level = jnp.broadcast_to(jnp.where(level_index < LEVELS - 1, level_index + 1, LEVELS)[None, :, None], (device_count, LEVELS, 1))
    source = (index_of_device[:, None] - neighbour_offsets()[None, :]) % device_count
    remote = jnp.where(level_index[None, :, None] < shared_depth[:, None, :], LEVELS + 1 + source[:, None, :] * GHOST_DEPTH + level_index[None, :, None], LEVELS)
    column_table = jnp.concatenate([own_level, upper_level, lower_level, remote], -1)
    return column_table.reshape(device_count * LEVELS, NEIGHBOURS).astype(jnp.int32)


def column_layout(key):
    device_count = COLUMNS // DEVICE_COLUMNS
    total_slot_count = device_count * SLOTS
    base_key = jax.random.fold_in(key, 23)
    dry_column = jax.random.randint(jax.random.fold_in(base_key, 1), (device_count, DEVICE_COLUMNS), 0, 10) < 3
    column_depth = jax.random.randint(jax.random.fold_in(base_key, 2), (device_count, DEVICE_COLUMNS), 1, LEVELS + 1)
    selected_source = jax.random.randint(jax.random.fold_in(base_key, 3), (), 0, device_count)
    selected_target = jax.random.randint(jax.random.fold_in(base_key, 4), (), 0, device_count)
    split_keys = jax.random.split(jax.random.fold_in(base_key, 5), device_count)
    rating_values = jax.vmap(lambda one_key: jax.random.permutation(one_key, total_slot_count))(split_keys)
    block_of_slots = jnp.arange(total_slot_count, dtype=jnp.int32) // SLOTS
    index_of_device = jnp.arange(device_count, dtype=jnp.int32)
    extra_credit = jnp.where((index_of_device[:, None] == selected_source) & (block_of_slots[None, :] == selected_target), total_slot_count, 0)
    ordering_of_slots = jnp.argsort(-(rating_values + extra_credit), axis=1, stable=True)[:, :DEVICE_COLUMNS]
    forced = (index_of_device[:, None] == selected_source) & (jnp.arange(DEVICE_COLUMNS, dtype=jnp.int32)[None, :] < SLOTS)
    wet_count = jnp.where(dry_column & jnp.logical_not(forced), 0, column_depth)
    column_of_slot = jax.vmap(lambda placed: jnp.full((total_slot_count,), DEVICE_COLUMNS, jnp.int32).at[placed].set(jnp.arange(DEVICE_COLUMNS, dtype=jnp.int32)))(ordering_of_slots)
    clipped = jnp.minimum(column_of_slot, DEVICE_COLUMNS - 1)
    alive_slot = (column_of_slot < DEVICE_COLUMNS) & (jnp.take_along_axis(wet_count, clipped, 1) > 0)
    slot_table = jnp.where(alive_slot, column_of_slot, DEVICE_COLUMNS)
    return (wet_count.reshape(device_count * DEVICE_COLUMNS).astype(jnp.int32), slot_table.reshape(device_count * device_count, SLOTS).astype(jnp.int32))


def draw_wet_levels(key, part):
    return column_layout(key)[0]


def draw_column_slots(key, part):
    return column_layout(key)[1]


def random_tiles(key, tile_shape):
    entries = jax.random.normal(key, tile_shape, jnp.float32)
    return entries


def draw_explicit_tiles(key, part):
    device_count = COLUMNS // DEVICE_COLUMNS
    tile_shape = (device_count * LEVELS, NEIGHBOURS, DEVICE_COLUMNS, DEVICE_COLUMNS)
    entries = random_tiles(jax.random.fold_in(key, 31), tile_shape) * (0.5 / math.sqrt(NEIGHBOURS * DEVICE_COLUMNS))
    entries = entries.at[:, 0].add(0.7 * jnp.eye(DEVICE_COLUMNS, dtype=jnp.float32))
    return entries.astype(jnp.bfloat16)


def draw_implicit_tiles(key, part):
    device_count = COLUMNS // DEVICE_COLUMNS
    tile_shape = (device_count * LEVELS, 3, DEVICE_COLUMNS, DEVICE_COLUMNS)
    entries = random_tiles(jax.random.fold_in(key, 37), tile_shape) * (0.4 / math.sqrt(3 * DEVICE_COLUMNS))
    entries = entries.at[:, 1].add(0.8 * jnp.eye(DEVICE_COLUMNS, dtype=jnp.float32))
    return entries.astype(jnp.bfloat16)


def shard_levels(rng, shape, pieces, low, largest):
    def one(position, blocks):
        steps = jax.random.uniform(jax.random.fold_in(jax.random.fold_in(rng, 6), position), (blocks,), jnp.float32, low / len(pieces), largest / len(pieces))
        return jnp.repeat(jnp.exp(steps), shape[position] // blocks).reshape((-1,) + (1,) * (len(shape) - position - 1))

    gain = one(*pieces[0])
    for cut in pieces[1:]:
        gain = gain * one(*cut)
    return gain


def noise(key, extent, spread, most, cuts=(), kind=jnp.bfloat16):
    values = spread * jax.random.normal(key, extent, jnp.float32)
    if cuts:
        values = values * shard_levels(key, extent, cuts, -0.22, 0.18)
    return jnp.clip(values, -most, most).astype(kind)


def setup_inputs(seed: int = 0, part: int = 0) -> dict:
    key_of = jax.random.split(jax.random.key(seed), 11)
    part_splits = jax.random.split(jax.random.fold_in(key_of[10], part), 11)
    return {
        "tracer_state": noise(part_splits[0], (TRACERS, LEVELS, COLUMNS), 1.0, 6.0, ((2, 16),), jnp.float32),
        "krylov_direction": noise(part_splits[1], (TRACERS, LEVELS, COLUMNS), 1.0, 6.0, ((2, 16),), jnp.float32),
        "explicit_tiles": draw_explicit_tiles(jax.random.fold_in(key_of[10], 71), part),
        "implicit_tiles": draw_implicit_tiles(jax.random.fold_in(key_of[10], 71), part),
        "explicit_columns": draw_explicit_columns(jax.random.fold_in(key_of[10], 71), part),
        "ghost_levels": draw_ghost_levels(jax.random.fold_in(key_of[10], 71), part),
        "wet_levels": draw_wet_levels(jax.random.fold_in(key_of[10], 71), part),
        "surface_light": jnp.clip(jnp.exp(math.log(4.0) - 2.7725887 * jax.random.uniform(part_splits[7], (COLUMNS,), jnp.float32) ** shard_levels(part_splits[7], (COLUMNS,), ((0, 16),), -0.2, 0.2)), 0.25, 4.0),
        "martin_exponent": jnp.clip(jnp.exp(math.log(2.0) - 1.3862944 * jax.random.uniform(part_splits[8], (COLUMNS,), jnp.float32) ** shard_levels(part_splits[8], (COLUMNS,), ((0, 16),), -0.2, 0.2)), 0.5, 2.0),
        "column_slots": draw_column_slots(jax.random.fold_in(key_of[10], 71), part),
    }


max_uptake = 1.0
half_saturation = 0.5
dop_fraction = 0.67
dop_decay = 0.2
time_step = 0.5


def sources(phosphate, organic, depth_count, surface_light, martin_exponent):
    levels = jnp.arange(phosphate.shape[0], dtype=jnp.float32)[:, None]
    wet_mask = (levels < depth_count[None, :]).astype(jnp.float32)
    sunlit = (levels < EUPHOTIC).astype(jnp.float32)
    depth_ratio = (levels + 1.0) ** 1.5 / (EUPHOTIC * 1.0) ** 1.5
    reaching = jnp.where(levels >= EUPHOTIC - 1, jnp.exp(-martin_exponent[None, :] * jnp.log(depth_ratio)), 1.0)
    passing = reaching * (levels < depth_count[None, :] - 1.0).astype(jnp.float32)
    passing_above = jnp.concatenate([jnp.ones_like(passing[:1]), passing[:-1]], 0)
    squared = phosphate * phosphate
    uptake = max_uptake * surface_light[None, :] * jnp.exp(-2.0 * levels / EUPHOTIC) * sunlit * wet_mask * squared / (half_saturation ** 2 + squared)
    export = (1.0 - dop_fraction) * jnp.sum(uptake, 0)
    remineral = export[None, :] * (passing_above - passing)
    decayed = dop_decay * organic * wet_mask
    return -uptake + decayed + remineral, dop_fraction * uptake - decayed, export


def column_sources(columns, params):
    def column_rates(phosphate, organic):
        return sources(phosphate, organic, params[0], params[1], params[2])

    primal, tangent = jax.jvp(column_rates, (columns[:, 0], columns[:, 1]), (columns[:, 2], columns[:, 3]))
    return jnp.stack([primal[0], primal[1], tangent[0], tangent[1]], 1), primal[2]


def explicit_index(explicit_columns, ghost_levels):
    row_count = explicit_columns.shape[0]
    device = (jnp.arange(row_count, dtype=jnp.int32) // LEVELS)[:, None]
    ghost_offset = explicit_columns - LEVELS - 1
    source = jnp.clip(ghost_offset // GHOST_DEPTH, 0, N_TILE - 1).astype(jnp.int32)
    ghost_slot = jnp.clip(ghost_offset % GHOST_DEPTH, 0, GHOST_DEPTH - 1).astype(jnp.int32)
    source_level = ghost_levels[source * N_TILE + device, ghost_slot]
    empty_index = N_TILE * LEVELS
    remote = jnp.where(source_level == LEVELS, empty_index, source * LEVELS + source_level)
    local_index = jnp.where(explicit_columns == LEVELS, empty_index, device * LEVELS + explicit_columns)
    return jnp.where(explicit_columns <= LEVELS, local_index, remote).astype(jnp.int32)


def reference(tracer_state, krylov_direction, explicit_tiles, implicit_tiles, explicit_columns, ghost_levels, wet_levels, surface_light, martin_exponent, column_slots):
    columns = tracer_state.shape[2]
    devices = columns // DEVICE_COLUMNS
    channels = 2 * TRACERS
    depth_count = wet_levels.astype(jnp.float32)
    params = jnp.stack([depth_count, surface_light, martin_exponent])
    wet_mask = (jnp.arange(LEVELS, dtype=jnp.float32)[:, None] < depth_count[None, :]).astype(jnp.float32)
    fields = jnp.concatenate([tracer_state, krylov_direction], 0).transpose(1, 0, 2)
    tile_index = explicit_index(explicit_columns, ghost_levels).reshape(devices, LEVELS, NEIGHBOURS)
    explicit_blocks = explicit_tiles.reshape(devices, LEVELS, NEIGHBOURS, DEVICE_COLUMNS, DEVICE_COLUMNS)
    implicit_blocks = implicit_tiles.reshape(devices, LEVELS, 3, DEVICE_COLUMNS, DEVICE_COLUMNS)

    def to_tiles(values):
        return values.reshape(LEVELS, channels, devices, DEVICE_COLUMNS).transpose(2, 0, 1, 3)

    def from_tiles(values):
        return values.transpose(1, 2, 0, 3).reshape(LEVELS, channels, columns)

    export_total = jnp.zeros((columns,), jnp.float32)
    for time_index in range(STEPS):
        source_rates, export = column_sources(fields, params)
        export_total = export_total + export
        rounded = to_tiles(fields.astype(jnp.bfloat16)).reshape(devices * LEVELS, channels, DEVICE_COLUMNS)
        rounded = jnp.concatenate([rounded, jnp.zeros((1, channels, DEVICE_COLUMNS), jnp.bfloat16)], 0)

        def apply_explicit(operand_pair):
            where_from, blocks = operand_pair
            return jnp.einsum("lkcj,lkji->lci", rounded[where_from].astype(jnp.float32), blocks.astype(jnp.float32))

        carried = lax.map(apply_explicit, (tile_index, explicit_blocks))
        intermediate = (carried + time_step * to_tiles(source_rates)).astype(jnp.bfloat16)
        padded = jnp.pad(intermediate, ((0, 0), (1, 1), (0, 0), (0, 0)))
        stacked = jnp.stack([padded[:, :-2], padded[:, 1:-1], padded[:, 2:]], 2)

        def apply_implicit(operand_pair):
            above_below, blocks = operand_pair
            return jnp.einsum("lkcj,lkji->lci", above_below.astype(jnp.float32), blocks.astype(jnp.float32))

        settled = lax.map(apply_implicit, (stacked, implicit_blocks))
        fields = wet_mask[:, None, :] * from_tiles(settled)
    slot_table = column_slots.reshape(devices, devices, -1).transpose(1, 0, 2)
    source_device = jnp.arange(devices, dtype=jnp.int32)[None, :, None]
    clipped = jnp.minimum(slot_table, DEVICE_COLUMNS - 1).astype(jnp.int32)
    picked = export_total[source_device * DEVICE_COLUMNS + clipped]
    export_flux = jnp.where(slot_table < DEVICE_COLUMNS, picked, 0.0).reshape(-1)
    result = fields.transpose(1, 0, 2)
    return result[:TRACERS], result[TRACERS:], export_flux
```

```python
import functools

import jax
import jax.numpy as jnp
from jax import lax
from jax.experimental import pallas as pl
from jax.experimental.pallas import tpu as pltpu
from jax.sharding import PartitionSpec as P

EUPHOTIC = 6
STEPS = 3

max_uptake = 1.0
half_saturation = 0.5
dop_fraction = 0.67
dop_decay = 0.2
time_step = 0.5

F32 = jnp.float32
BF16 = jnp.bfloat16
MIB = 1 << 20

CHANNELS = 4
PAIR = 2 * CHANNELS
QUAD = 4 * CHANNELS
EDGE = PAIR


class Sizes:
    def __init__(self, levels, columns, depth):
        self.levels = levels
        self.columns = columns
        self.depth = depth
        self.pairs = levels // 2
        self.quads = (levels + 3) // 4
        self.rows = QUAD * self.quads
        self.padded = self.rows + 2 * EDGE
        self.ghost_pairs = (depth + 1) // 2
        self.low_pairs = min((depth + 2) // 2, self.pairs)
        self.ghost_quads = (self.ghost_pairs + 1) // 2
        self.low_quads = (self.low_pairs + 1) // 2
        self.send_rows = QUAD * self.ghost_quads
        self.low_rows = PAIR * self.low_pairs
        self.high_rows = PAIR * (self.pairs - self.low_pairs)


def sublane(columns):
    return lax.broadcasted_iota(jnp.int32, (PAIR, columns), 0)


def tiles_of(ref, level, columns):
    return ref[level].reshape(3 * columns, columns)


def pair_product(lhs, ref, pair, columns):
    rhs = jnp.concatenate(
        [tiles_of(ref, 2 * pair, columns), tiles_of(ref, 2 * pair + 1, columns)], axis=1
    )
    product = jnp.dot(lhs, rhs, preferred_element_type=F32)
    top = PAIR * (pair % 2)
    upper = product[top : top + PAIR, :columns]
    lower = product[top : top + PAIR, columns:]
    return jnp.where(sublane(columns) < CHANNELS, upper, lower)


def window(ref, start, offsets):
    parts = [ref[start + offset : start + offset + QUAD, :] for offset in offsets]
    return jnp.concatenate(parts, axis=1).astype(BF16)


def wet_rows(pair, wet, columns):
    return (2 * pair + sublane(columns) // CHANNELS) < wet


def uptake_of(ref, base, wet, light, columns):
    level = lax.broadcasted_iota(jnp.int32, (PAIR, columns), 0)
    phosphate = ref[pl.ds(base, PAIR, stride=CHANNELS), :]
    direction = ref[pl.ds(base + 2, PAIR, stride=CHANNELS), :]
    scale = max_uptake * light * jnp.exp(-2.0 * level.astype(F32) / EUPHOTIC)
    scale = jnp.where((level < EUPHOTIC) & (level < wet), scale, 0.0)
    squared = phosphate * phosphate
    half = half_saturation**2
    inverse = 1.0 / (half + squared)
    uptake = scale * squared * inverse
    slope = scale * half * (2.0 * phosphate * direction) * inverse * inverse
    return uptake, slope


def passing_at(level, wet, exponent):
    ratio = (level + 1).astype(F32) / EUPHOTIC
    ratio = jnp.maximum(ratio, 1.0)
    reaching = jnp.where(level >= EUPHOTIC - 1, jnp.exp(-1.5 * exponent * jnp.log(ratio)), 1.0)
    return jnp.where(level < wet - 1, reaching, 0.0)


def prepare_kernel(size, state_ref, krylov_ref, low_ref, high_ref, send_ref, fields_ref):
    fields_ref[...] = jnp.zeros_like(fields_ref)
    for channel in range(CHANNELS):
        source = state_ref if channel < 2 else krylov_ref
        fields_ref[pl.ds(channel, size.levels, stride=CHANNELS), :] = source[:, channel % 2, :]
    low_ref[...] = fields_ref[: size.low_rows, :]
    high_ref[...] = fields_ref[size.low_rows : size.low_rows + size.high_rows, :]
    send_ref[...] = fields_ref[: size.send_rows, :].astype(BF16)


def chunks_of(size):
    cuts = [size.quads * k // 3 for k in range(4)]
    return [(4 * a, min(4 * b, size.levels)) for a, b in zip(cuts, cuts[1:])]


def weight_copies(size, explicit_hbm, implicit_hbm, own_ref, ghost_ref, implicit_ref, semaphore):
    copies = []
    low = 2 * size.low_pairs

    def add(source, target):
        copies.append(pltpu.make_async_copy(source, target, semaphore.at[len(copies)]))

    for start, stop in chunks_of(size):
        part = pl.ds(start, stop - start)
        add(explicit_hbm.at[part, pl.ds(0, 3)], own_ref.at[part])
    part = pl.ds(low, size.levels - low)
    add(implicit_hbm.at[part], implicit_ref.at[part])
    part = pl.ds(0, 2 * size.ghost_pairs)
    add(explicit_hbm.at[part, pl.ds(3, 3)], ghost_ref)
    part = pl.ds(0, low)
    add(implicit_hbm.at[part], implicit_ref.at[part])
    return copies


def local_kernel(size, stage, slots, *refs):
    low_ref, high_ref, wet_ref, light_ref = refs[:4]
    copies = None
    if stage == "first":
        exponent_ref, columns_ref, explicit_hbm, implicit_hbm = refs[4:8]
        partial_ref, next_high_ref, total_ref, remineral_ref, depth_ref = refs[8:13]
        own_ref, ghost_ref, implicit_ref = refs[13:16]
        fields_ref, middle_ref, rate_ref, semaphore = refs[16:]
        copies = weight_copies(
            size, explicit_hbm, implicit_hbm, own_ref, ghost_ref, implicit_ref, semaphore
        )
        for copy in copies:
            copy.start()
    else:
        remineral_ref, total_in_ref, own_ref, implicit_ref = refs[4:8]
        if stage == "last":
            slots_ref, partial_ref, next_high_ref, payload_ref = refs[8:12]
        else:
            partial_ref, next_high_ref, total_ref = refs[8:11]
        fields_ref, middle_ref, rate_ref = refs[-3:]
    columns = size.columns
    wet = wet_ref[...]
    light = light_ref[...]
    zero_edge = jnp.zeros((EDGE, columns), F32)
    live = PAIR * size.pairs
    for ref in (fields_ref, middle_ref):
        ref[:EDGE, :] = zero_edge
        for start in range(EDGE + live, size.padded, PAIR):
            ref[start : start + PAIR, :] = zero_edge
    fields_ref[EDGE : EDGE + size.low_rows, :] = low_ref[...]
    fields_ref[EDGE + size.low_rows : EDGE + live, :] = high_ref[...]
    if stage == "first":
        exponent = exponent_ref[...]
        level = lax.broadcasted_iota(jnp.int32, (size.rows // CHANNELS, columns), 0)
        above = jnp.where(level == 0, 1.0, passing_at(level - 1, wet, exponent))
        share = time_step * (above - passing_at(level, wet, exponent))
        blank = jnp.zeros_like(share)
        for channel in range(CHANNELS):
            remineral_ref[pl.ds(channel, size.rows // CHANNELS, stride=CHANNELS), :] = (
                blank if channel % 2 else share
            )
        here = (columns_ref[...] != size.levels).astype(F32)
        depth = jnp.sum(here, axis=1, keepdims=True).astype(jnp.int32)
        depth_ref[...] = jnp.broadcast_to(depth, depth_ref.shape)
    uptake, slope = uptake_of(fields_ref, EDGE, wet, light, columns)
    export = (1.0 - dop_fraction) * jnp.sum(uptake, axis=0, keepdims=True)
    export_slope = (1.0 - dop_fraction) * jnp.sum(slope, axis=0, keepdims=True)
    total = export if stage == "first" else total_in_ref[...] + export
    if stage == "last":
        targets, _, width = payload_ref.shape
        column = lax.broadcasted_iota(jnp.int32, (targets, columns), 1)
        lane = lax.broadcasted_iota(jnp.int32, (targets, width), 1) - slots * lax.axis_index("tile")
        payload = jnp.zeros((targets, width), F32)
        for slot in range(slots):
            chosen = column == slots_ref[:, slot : slot + 1]
            value = jnp.sum(jnp.where(chosen, total, 0.0), axis=1, keepdims=True)
            payload = jnp.where(lane == slot, value, payload)
        payload_ref[:, 0, :] = payload
    else:
        total_ref[...] = total
    for channel, rate in enumerate((uptake, uptake, slope, slope)):
        factor = time_step * (dop_fraction if channel % 2 else -1.0)
        rate_ref[pl.ds(channel, PAIR, stride=CHANNELS), :] = factor * rate
    row = sublane(columns)
    sinking = jnp.where(row % CHANNELS < 2, export, export_slope)
    organic_row = row % 2 == 1

    def sources(pair):
        top = PAIR * pair
        own = fields_ref[EDGE + top : EDGE + top + PAIR, :]
        following = fields_ref[EDGE + top + 1 : EDGE + top + PAIR + 1, :]
        decayed = (time_step * dop_decay) * jnp.where(organic_row, -own, following)
        rate = jnp.where(wet_rows(pair, wet, columns), decayed, 0.0)
        rate = rate + remineral_ref[top : top + PAIR, :] * sinking
        if top < CHANNELS * PAIR:
            rate = rate + rate_ref[top : top + PAIR, :]
        return rate

    arrivals = {start // 4: place for place, (start, _) in enumerate(chunks_of(size))}
    for quad in range(size.quads):
        if copies and quad in arrivals:
            copies[arrivals[quad]].wait()
        lhs = window(fields_ref, EDGE + QUAD * quad, (0, -CHANNELS, CHANNELS))
        for pair in range(2 * quad, min(2 * quad + 2, size.pairs)):
            top = PAIR * pair
            value = pair_product(lhs, own_ref, pair, columns) + sources(pair)
            partial_ref[top : top + PAIR, :] = value
            middle_ref[EDGE + top : EDGE + top + PAIR, :] = value
    for start in range(live, size.rows, PAIR):
        partial_ref[start : start + PAIR, :] = zero_edge
    if copies:
        copies[-3].wait()
    for quad in range(size.low_pairs // 2, size.quads):
        lhs = window(middle_ref, EDGE + QUAD * quad, (-CHANNELS, 0, CHANNELS))
        for pair in range(max(2 * quad, size.low_pairs), min(2 * quad + 2, size.pairs)):
            settled = pair_product(lhs, implicit_ref, pair, columns)
            top = PAIR * (pair - size.low_pairs)
            next_high_ref[top : top + PAIR, :] = jnp.where(
                wet_rows(pair, wet, columns), settled, 0.0
            )
    if copies:
        copies[-2].wait()
        copies[-1].wait()


def ghost_kernel(size, last, *refs):
    partial_ref, pair_ref, other_ref, across_ref, depth_ref, wet_ref = refs[:6]
    if last:
        explicit_hbm, implicit_hbm, high_ref = refs[6:9]
        state_ref, tangent_ref, middle_ref, fields_ref, ghost_ref, implicit_ref, semaphore = refs[9:]
        low = pl.ds(0, 2 * size.low_pairs)
        part = pl.ds(0, 2 * size.ghost_pairs)
        copies = [
            pltpu.make_async_copy(
                explicit_hbm.at[part, pl.ds(3, 3)], ghost_ref, semaphore.at[0]
            ),
            pltpu.make_async_copy(implicit_hbm.at[low], implicit_ref, semaphore.at[1]),
        ]
        for copy in copies:
            copy.start()
    else:
        ghost_ref, implicit_ref, low_ref, send_ref, middle_ref = refs[6:]
    columns = size.columns
    wet = wet_ref[...]
    even = lax.axis_index("tile") % 2 == 0
    middle_ref[:EDGE, :] = jnp.zeros((EDGE, columns), F32)
    for top in range(PAIR * size.ghost_pairs, QUAD * size.low_quads + EDGE, PAIR):
        middle_ref[EDGE + top : EDGE + top + PAIR, :] = partial_ref[top : top + PAIR, :]
    if last:
        copies[0].wait()
    for quad in range(size.ghost_quads):
        span = slice(QUAD * quad, QUAD * quad + QUAD)
        own_chip = pair_ref[span, :].astype(F32)
        next_chip = other_ref[span, :].astype(F32)
        across = across_ref[span, :].astype(F32)
        level = lax.broadcasted_iota(jnp.int32, (QUAD, columns), 0) // CHANNELS + CHANNELS * quad
        before = jnp.where(even, next_chip, own_chip)
        after = jnp.where(even, own_chip, next_chip)
        before = jnp.where(level < depth_ref[3:4, :], before, 0.0)
        after = jnp.where(level < depth_ref[4:5, :], after, 0.0)
        across = jnp.where(level < depth_ref[5:6, :], across, 0.0)
        lhs = jnp.concatenate([before, after, across], axis=1).astype(BF16)
        for pair in range(2 * quad, min(2 * quad + 2, size.ghost_pairs)):
            top = PAIR * pair
            value = pair_product(lhs, ghost_ref, pair, columns)
            middle_ref[EDGE + top : EDGE + top + PAIR, :] = value + partial_ref[top : top + PAIR, :]
    if last:
        copies[1].wait()
    values = []
    for quad in range(size.low_quads):
        lhs = window(middle_ref, EDGE + QUAD * quad, (-CHANNELS, 0, CHANNELS))
        for pair in range(2 * quad, min(2 * quad + 2, size.low_pairs)):
            settled = pair_product(lhs, implicit_ref, pair, columns)
            values.append(jnp.where(wet_rows(pair, wet, columns), settled, 0.0))
    if last:
        for pair, value in enumerate(values):
            fields_ref[PAIR * pair : PAIR * pair + PAIR, :] = value
        fields_ref[size.low_rows : size.low_rows + size.high_rows, :] = high_ref[...]
        for channel in range(CHANNELS):
            out_ref = state_ref if channel < 2 else tangent_ref
            out_ref[:, channel % 2, :] = fields_ref[pl.ds(channel, size.levels, stride=CHANNELS), :]
        return
    for pair, value in enumerate(values):
        low_ref[PAIR * pair : PAIR * pair + PAIR, :] = value
    blank = jnp.zeros((PAIR, columns), F32)
    for quad in range(size.ghost_quads):
        two = [
            values[pair] if pair < len(values) else blank for pair in (2 * quad, 2 * quad + 1)
        ]
        send_ref[QUAD * quad : QUAD * quad + QUAD, :] = jnp.concatenate(two, axis=0).astype(BF16)


def gather_kernel(arrived_ref, flux_ref):
    flux = jnp.sum(arrived_ref[:, 0, :], axis=0, keepdims=True)
    flux_ref[...] = flux[:, : flux_ref.shape[1]]


def call(body, name, outputs, scratch, operands, flops=1000000, in_hbm=()):
    space = lambda place: pltpu.HBM if place in in_hbm else pltpu.VMEM
    operands = [
        pltpu.with_memory_space_constraint(value, pltpu.HBM) if place in in_hbm else value
        for place, value in enumerate(operands)
    ]
    return pl.pallas_call(
        body,
        name=name,
        out_shape=outputs,
        in_specs=[pl.BlockSpec(memory_space=space(k)) for k in range(len(operands))],
        out_specs=[pl.BlockSpec(memory_space=pltpu.VMEM)] * len(outputs),
        scratch_shapes=scratch,
        compiler_params=pltpu.CompilerParams(vmem_limit_bytes=8 * MIB),
        cost_estimate=pl.CostEstimate(flops=flops, bytes_accessed=100000, transcendentals=0),
    )(*operands)


def on_device(
    tracer_state,
    krylov_direction,
    explicit_tiles,
    implicit_tiles,
    explicit_columns,
    ghost_levels,
    wet_levels,
    surface_light,
    martin_exponent,
    column_slots,
):
    size = Sizes(tracer_state.shape[1], tracer_state.shape[2], ghost_levels.shape[1])
    columns = size.columns
    tile_count = lax.axis_size("tile")
    slots = column_slots.shape[1]
    width = -(-tile_count * slots // 128) * 128
    row_of = lambda value: value.reshape(1, columns)
    wet, light, exponent = row_of(wet_levels), row_of(surface_light), row_of(martin_exponent)

    same_chip = [(d, d ^ 1) for d in range(tile_count)]
    next_chip = [(d, (d + (1 if d % 2 else -1)) % tile_count) for d in range(tile_count)]
    opposite = [(d, (d + tile_count // 2) % tile_count) for d in range(tile_count)]

    def exchange(value):
        across = lax.ppermute(value, "tile", opposite)
        other = lax.ppermute(value, "tile", next_chip)
        pair = lax.ppermute(value, "tile", same_chip)
        return pair, other, across

    def shape(rows, dtype=F32):
        return pltpu.VMEM((rows, columns), dtype)

    def tiles(levels):
        return pltpu.VMEM((levels, 3, columns, columns), BF16)

    padded = pltpu.VMEM((size.padded, columns), F32)
    low_scratch = pltpu.VMEM((QUAD * size.low_quads + 2 * EDGE, columns), F32)
    local_scratch = [padded, padded, pltpu.VMEM((CHANNELS * PAIR, columns), F32)]
    depth_shape = pltpu.VMEM((explicit_columns.shape[1], columns), jnp.int32)

    low, high, send = call(
        functools.partial(prepare_kernel, size),
        "prepare",
        [shape(size.low_rows), shape(size.high_rows), shape(size.send_rows, BF16)],
        [pltpu.VMEM((size.rows, columns), F32)],
        [tracer_state.transpose(1, 0, 2), krylov_direction.transpose(1, 0, 2)],
    )
    for time_index in range(STEPS):
        first, last = time_index == 0, time_index == STEPS - 1
        ghosts = exchange(send)
        operands = [low, high, wet, light]
        outputs = [shape(size.rows), shape(size.high_rows)]
        if first:
            partial, high, total, remineral, depth, own, ghost, implicit = call(
                functools.partial(local_kernel, size, "first", slots),
                "local_first",
                outputs
                + [
                    shape(1),
                    shape(size.rows),
                    depth_shape,
                    tiles(size.levels),
                    tiles(2 * size.ghost_pairs),
                    tiles(size.levels),
                ],
                local_scratch + [pltpu.SemaphoreType.DMA((6,))],
                operands + [exponent, explicit_columns.T, explicit_tiles, implicit_tiles],
                8000000,
                (6, 7),
            )
        elif last:
            partial, high, payload = call(
                functools.partial(local_kernel, size, "last", slots),
                "local_last",
                outputs + [jax.ShapeDtypeStruct((tile_count, 1, width), F32)],
                local_scratch,
                operands + [remineral, total, own, implicit, column_slots],
                4000000,
            )
            arrived = lax.all_to_all(payload, "tile", split_axis=0, concat_axis=0, tiled=True)
        else:
            partial, high, total = call(
                functools.partial(local_kernel, size, "middle", slots),
                "local",
                outputs + [shape(1)],
                local_scratch,
                operands + [remineral, total, own, implicit],
                4000000,
            )
        operands = [partial, *ghosts, depth, wet]
        if last:
            tall = jax.ShapeDtypeStruct((size.levels, CHANNELS // 2, columns), F32)
            state_out, tangent_out = call(
                functools.partial(ghost_kernel, size, True),
                "ghost_last",
                [tall, tall],
                [
                    low_scratch,
                    pltpu.VMEM((size.rows, columns), F32),
                    tiles(2 * size.ghost_pairs),
                    tiles(2 * size.low_pairs),
                    pltpu.SemaphoreType.DMA((2,)),
                ],
                operands + [explicit_tiles, implicit_tiles, high],
                2000000,
                (6, 7),
            )
        else:
            low, send = call(
                functools.partial(ghost_kernel, size, False),
                "ghost",
                [shape(size.low_rows), shape(size.send_rows, BF16)],
                [low_scratch],
                operands + [ghost, implicit],
            )
    (flux,) = call(
        gather_kernel,
        "gather",
        [jax.ShapeDtypeStruct((1, tile_count * slots), F32)],
        [],
        [arrived],
    )
    return state_out.transpose(1, 0, 2), tangent_out.transpose(1, 0, 2), flux.reshape(-1)


def solution(mesh):
    return jax.shard_map(
        on_device,
        mesh=mesh,
        in_specs=(
            P(None, None, ("groups", "tile")),
            P(None, None, ("groups", "tile")),
            P("tile", None, None, None),
            P("tile", None, None, None),
            P("tile", None),
            P("tile", None),
            P("tile"),
            P(("groups", "tile")),
            P(("groups", "tile")),
            P("tile", None),
        ),
        out_specs=(
            P(None, None, ("groups", "tile")),
            P(None, None, ("groups", "tile")),
            P(("groups", "tile")),
        ),
        check_vma=False,
    )
```

```python
import functools

import jax
import jax.numpy as jnp
from jax import lax
from jax.experimental import pallas as pl
from jax.experimental.pallas import tpu as pltpu
from jax.sharding import PartitionSpec as P


EUPHOTIC = 6
STEPS = 3

max_uptake = 1.0
half_saturation = 0.5
dop_fraction = 0.67
dop_decay = 0.2
time_step = 0.5

F32 = jnp.float32
BF16 = jnp.bfloat16
MIB = 1 << 20
PREPARE_FLOPS = 10**10

CHANNELS = 4
PAIR = 2 * CHANNELS
QUAD = 4 * CHANNELS
EDGE = PAIR


class Sizes:
    def __init__(self, levels, columns, depth):
        self.levels = levels
        self.columns = columns
        self.pairs = levels // 2
        self.quads = (levels + 3) // 4
        self.rows = QUAD * self.quads
        self.padded = self.rows + 2 * EDGE
        self.ghost_pairs = (depth + 1) // 2
        self.low_pairs = min((depth + 2) // 2, self.pairs)
        self.ghost_quads = (self.ghost_pairs + 1) // 2
        self.low_quads = (self.low_pairs + 1) // 2
        self.send_rows = QUAD * self.ghost_quads
        self.low_rows = PAIR * self.low_pairs
        self.high_rows = PAIR * (self.pairs - self.low_pairs)


def sublane(columns):
    return lax.broadcasted_iota(jnp.int32, (PAIR, columns), 0)


def tiles_of(ref, level, first, columns):
    return ref[level, first : first + 3].reshape(3 * columns, columns)


def pair_product(lhs, ref, pair, columns, first=0):
    rhs = jnp.concatenate(
        [tiles_of(ref, 2 * pair, first, columns), tiles_of(ref, 2 * pair + 1, first, columns)],
        axis=1,
    )
    product = jnp.dot(lhs, rhs, preferred_element_type=F32)
    top = PAIR * (pair % 2)
    upper = product[top : top + PAIR, :columns]
    lower = product[top : top + PAIR, columns:]
    return jnp.where(sublane(columns) < CHANNELS, upper, lower)


def window(ref, start, offsets):
    parts = [ref[start + offset : start + offset + QUAD, :] for offset in offsets]
    return jnp.concatenate(parts, axis=1).astype(BF16)


def wet_rows(pair, wet, columns):
    return (2 * pair + sublane(columns) // CHANNELS) < wet


def uptake_of(ref, base, wet, light, columns):
    level = lax.broadcasted_iota(jnp.int32, (PAIR, columns), 0)
    phosphate = ref[pl.ds(base, PAIR, stride=CHANNELS), :]
    direction = ref[pl.ds(base + 2, PAIR, stride=CHANNELS), :]
    scale = max_uptake * light * jnp.exp(-2.0 * level.astype(F32) / EUPHOTIC)
    scale = jnp.where((level < EUPHOTIC) & (level < wet), scale, 0.0)
    squared = phosphate * phosphate
    half = half_saturation**2
    inverse = 1.0 / (half + squared)
    uptake = scale * squared * inverse
    slope = scale * half * (2.0 * phosphate * direction) * inverse * inverse
    return uptake, slope


def passing_at(level, wet, exponent):
    ratio = (level + 1).astype(F32) / EUPHOTIC
    ratio = jnp.maximum(ratio, 1.0)
    reaching = jnp.where(level >= EUPHOTIC - 1, jnp.exp(-1.5 * exponent * jnp.log(ratio)), 1.0)
    return jnp.where(level < wet - 1, reaching, 0.0)


def prepare_kernel(size, small, *refs):
    state_hbm, krylov_hbm = refs[:2]
    small_hbm = refs[2 : 2 + small]
    low_ref, high_ref, send_ref = refs[2 + small : 5 + small]
    small_refs = refs[5 + small : 5 + 2 * small]
    state_ref, krylov_ref, fields_ref, semaphore = refs[5 + 2 * small :]
    pairs = [(state_hbm, state_ref), (krylov_hbm, krylov_ref), *zip(small_hbm, small_refs)]
    copies = [
        pltpu.make_async_copy(source, target, semaphore.at[place])
        for place, (source, target) in enumerate(pairs)
    ]
    for copy in copies:
        copy.start()
    fields_ref[...] = jnp.zeros_like(fields_ref)
    copies[0].wait()
    copies[1].wait()
    for channel in range(CHANNELS):
        source = state_ref if channel < 2 else krylov_ref
        fields_ref[pl.ds(channel, size.levels, stride=CHANNELS), :] = source[:, channel % 2, :]
    low_ref[...] = fields_ref[: size.low_rows, :]
    high_ref[...] = fields_ref[size.low_rows : size.low_rows + size.high_rows, :]
    send_ref[...] = fields_ref[: size.send_rows, :].astype(BF16)
    for copy in copies[2:]:
        copy.wait()


def local_kernel(size, stage, slots, *refs):
    low_ref, high_ref, wet_ref, light_ref = refs[:4]
    if stage == "first":
        exponent_ref, columns_ref, explicit_ref, implicit_ref = refs[4:8]
        partial_ref, next_high_ref, total_ref, remineral_ref, depth_ref = refs[8:13]
        fields_ref, middle_ref, rate_ref = refs[13:]
    else:
        remineral_ref, total_in_ref, explicit_ref, implicit_ref = refs[4:8]
        if stage == "last":
            slots_ref, partial_ref, next_high_ref, payload_ref = refs[8:12]
        else:
            partial_ref, next_high_ref, total_ref = refs[8:11]
        fields_ref, middle_ref, rate_ref = refs[-3:]
    columns = size.columns
    wet = wet_ref[...]
    light = light_ref[...]
    zero_edge = jnp.zeros((EDGE, columns), F32)
    live = PAIR * size.pairs
    for ref in (fields_ref, middle_ref):
        ref[:EDGE, :] = zero_edge
        for start in range(EDGE + live, size.padded, PAIR):
            ref[start : start + PAIR, :] = zero_edge
    fields_ref[EDGE : EDGE + size.low_rows, :] = low_ref[...]
    fields_ref[EDGE + size.low_rows : EDGE + live, :] = high_ref[...]
    if stage == "first":
        exponent = exponent_ref[...]
        level = lax.broadcasted_iota(jnp.int32, (size.rows // CHANNELS, columns), 0)
        above = jnp.where(level == 0, 1.0, passing_at(level - 1, wet, exponent))
        share = time_step * (above - passing_at(level, wet, exponent))
        blank = jnp.zeros_like(share)
        for channel in range(CHANNELS):
            remineral_ref[pl.ds(channel, size.rows // CHANNELS, stride=CHANNELS), :] = (
                blank if channel % 2 else share
            )
        here = (columns_ref[...] != size.levels).astype(F32)
        depth = jnp.sum(here, axis=1, keepdims=True).astype(jnp.int32)
        depth_ref[...] = jnp.broadcast_to(depth, depth_ref.shape)
    uptake, slope = uptake_of(fields_ref, EDGE, wet, light, columns)
    export = (1.0 - dop_fraction) * jnp.sum(uptake, axis=0, keepdims=True)
    export_slope = (1.0 - dop_fraction) * jnp.sum(slope, axis=0, keepdims=True)
    total = export if stage == "first" else total_in_ref[...] + export
    if stage == "last":
        targets, _, width = payload_ref.shape
        column = lax.broadcasted_iota(jnp.int32, (targets, columns), 1)
        lane = lax.broadcasted_iota(jnp.int32, (targets, width), 1) - slots * lax.axis_index("tile")
        payload = jnp.zeros((targets, width), F32)
        for slot in range(slots):
            chosen = column == slots_ref[:, slot : slot + 1]
            value = jnp.sum(jnp.where(chosen, total, 0.0), axis=1, keepdims=True)
            payload = jnp.where(lane == slot, value, payload)
        payload_ref[:, 0, :] = payload
    else:
        total_ref[...] = total
    for channel, rate in enumerate((uptake, uptake, slope, slope)):
        factor = time_step * (dop_fraction if channel % 2 else -1.0)
        rate_ref[pl.ds(channel, PAIR, stride=CHANNELS), :] = factor * rate
    row = sublane(columns)
    sinking = jnp.where(row % CHANNELS < 2, export, export_slope)
    organic_row = row % 2 == 1

    def sources(pair):
        top = PAIR * pair
        own = fields_ref[EDGE + top : EDGE + top + PAIR, :]
        following = fields_ref[EDGE + top + 1 : EDGE + top + PAIR + 1, :]
        decayed = (time_step * dop_decay) * jnp.where(organic_row, -own, following)
        rate = jnp.where(wet_rows(pair, wet, columns), decayed, 0.0)
        rate = rate + remineral_ref[top : top + PAIR, :] * sinking
        if top < CHANNELS * PAIR:
            rate = rate + rate_ref[top : top + PAIR, :]
        return rate

    for quad in range(size.quads):
        lhs = window(fields_ref, EDGE + QUAD * quad, (0, -CHANNELS, CHANNELS))
        for pair in range(2 * quad, min(2 * quad + 2, size.pairs)):
            top = PAIR * pair
            value = pair_product(lhs, explicit_ref, pair, columns) + sources(pair)
            partial_ref[top : top + PAIR, :] = value
            middle_ref[EDGE + top : EDGE + top + PAIR, :] = value
    for start in range(live, size.rows, PAIR):
        partial_ref[start : start + PAIR, :] = zero_edge
    for quad in range(size.low_pairs // 2, size.quads):
        lhs = window(middle_ref, EDGE + QUAD * quad, (-CHANNELS, 0, CHANNELS))
        for pair in range(max(2 * quad, size.low_pairs), min(2 * quad + 2, size.pairs)):
            settled = pair_product(lhs, implicit_ref, pair, columns)
            top = PAIR * (pair - size.low_pairs)
            next_high_ref[top : top + PAIR, :] = jnp.where(
                wet_rows(pair, wet, columns), settled, 0.0
            )


def ghost_kernel(size, last, *refs):
    partial_ref, pair_ref, other_ref, across_ref, depth_ref, wet_ref = refs[:6]
    if last:
        explicit_hbm, implicit_hbm, high_ref = refs[6:9]
        state_ref, tangent_ref, middle_ref, fields_ref, ghost_ref, implicit_ref, semaphore = refs[9:]
        low = pl.ds(0, 2 * size.low_pairs)
        part = pl.ds(0, 2 * size.ghost_pairs)
        copies = [
            pltpu.make_async_copy(
                explicit_hbm.at[part, pl.ds(3, 3)], ghost_ref, semaphore.at[0]
            ),
            pltpu.make_async_copy(implicit_hbm.at[low], implicit_ref, semaphore.at[1]),
        ]
        for copy in copies:
            copy.start()
        first = 0
    else:
        ghost_ref, implicit_ref, low_ref, send_ref, middle_ref = refs[6:]
        first = 3
    columns = size.columns
    wet = wet_ref[...]
    even = lax.axis_index("tile") % 2 == 0
    middle_ref[:EDGE, :] = jnp.zeros((EDGE, columns), F32)
    for top in range(PAIR * size.ghost_pairs, QUAD * size.low_quads + EDGE, PAIR):
        middle_ref[EDGE + top : EDGE + top + PAIR, :] = partial_ref[top : top + PAIR, :]
    if last:
        copies[0].wait()
    for quad in range(size.ghost_quads):
        span = slice(QUAD * quad, QUAD * quad + QUAD)
        own_chip = pair_ref[span, :].astype(F32)
        next_chip = other_ref[span, :].astype(F32)
        across = across_ref[span, :].astype(F32)
        level = lax.broadcasted_iota(jnp.int32, (QUAD, columns), 0) // CHANNELS + CHANNELS * quad
        before = jnp.where(even, next_chip, own_chip)
        after = jnp.where(even, own_chip, next_chip)
        before = jnp.where(level < depth_ref[3:4, :], before, 0.0)
        after = jnp.where(level < depth_ref[4:5, :], after, 0.0)
        across = jnp.where(level < depth_ref[5:6, :], across, 0.0)
        lhs = jnp.concatenate([before, after, across], axis=1).astype(BF16)
        for pair in range(2 * quad, min(2 * quad + 2, size.ghost_pairs)):
            top = PAIR * pair
            value = pair_product(lhs, ghost_ref, pair, columns, first)
            middle_ref[EDGE + top : EDGE + top + PAIR, :] = value + partial_ref[top : top + PAIR, :]
    if last:
        copies[1].wait()
    values = []
    for quad in range(size.low_quads):
        lhs = window(middle_ref, EDGE + QUAD * quad, (-CHANNELS, 0, CHANNELS))
        for pair in range(2 * quad, min(2 * quad + 2, size.low_pairs)):
            settled = pair_product(lhs, implicit_ref, pair, columns)
            values.append(jnp.where(wet_rows(pair, wet, columns), settled, 0.0))
    if last:
        for pair, value in enumerate(values):
            fields_ref[PAIR * pair : PAIR * pair + PAIR, :] = value
        fields_ref[size.low_rows : size.low_rows + size.high_rows, :] = high_ref[...]
        for channel in range(CHANNELS):
            out_ref = state_ref if channel < 2 else tangent_ref
            out_ref[:, channel % 2, :] = fields_ref[pl.ds(channel, size.levels, stride=CHANNELS), :]
        return
    for pair, value in enumerate(values):
        low_ref[PAIR * pair : PAIR * pair + PAIR, :] = value
    blank = jnp.zeros((PAIR, columns), F32)
    for quad in range(size.ghost_quads):
        two = [
            values[pair] if pair < len(values) else blank for pair in (2 * quad, 2 * quad + 1)
        ]
        send_ref[QUAD * quad : QUAD * quad + QUAD, :] = jnp.concatenate(two, axis=0).astype(BF16)


def gather_kernel(arrived_ref, flux_ref):
    flux = jnp.sum(arrived_ref[:, 0, :], axis=0, keepdims=True)
    flux_ref[...] = flux[:, : flux_ref.shape[1]]


def in_vmem(value):
    return pltpu.with_memory_space_constraint(value, pltpu.VMEM)


def call(body, outputs, scratch, operands, flops=1000000, in_hbm=()):
    space = lambda place: pltpu.HBM if place in in_hbm else pltpu.VMEM
    operands = [
        pltpu.with_memory_space_constraint(value, pltpu.HBM) if place in in_hbm else value
        for place, value in enumerate(operands)
    ]
    return pl.pallas_call(
        body,
        out_shape=outputs,
        in_specs=[pl.BlockSpec(memory_space=space(k)) for k in range(len(operands))],
        out_specs=[pl.BlockSpec(memory_space=pltpu.VMEM)] * len(outputs),
        scratch_shapes=scratch,
        compiler_params=pltpu.CompilerParams(vmem_limit_bytes=8 * MIB),
        cost_estimate=pl.CostEstimate(flops=flops, bytes_accessed=100000, transcendentals=0),
    )(*operands)


def on_device(
    tracer_state,
    krylov_direction,
    explicit_tiles,
    implicit_tiles,
    explicit_columns,
    ghost_levels,
    wet_levels,
    surface_light,
    martin_exponent,
    column_slots,
):
    size = Sizes(tracer_state.shape[1], tracer_state.shape[2], ghost_levels.shape[1])
    columns = size.columns
    tile_count = lax.axis_size("tile")
    slots = column_slots.shape[1]
    width = -(-tile_count * slots // 128) * 128
    row_of = lambda value: value.reshape(1, columns)
    explicit, implicit = in_vmem(explicit_tiles), in_vmem(implicit_tiles)

    same_chip = [(d, d ^ 1) for d in range(tile_count)]
    next_chip = [(d, (d + (1 if d % 2 else -1)) % tile_count) for d in range(tile_count)]
    opposite = [(d, (d + tile_count // 2) % tile_count) for d in range(tile_count)]

    def exchange(value):
        across = lax.ppermute(value, "tile", opposite)
        other = lax.ppermute(value, "tile", next_chip)
        pair = lax.ppermute(value, "tile", same_chip)
        return pair, other, across

    def shape(rows, dtype=F32):
        return pltpu.VMEM((rows, columns), dtype)

    def tiles(levels):
        return pltpu.VMEM((levels, 3, columns, columns), BF16)

    padded = pltpu.VMEM((size.padded, columns), F32)
    low_scratch = pltpu.VMEM((QUAD * size.low_quads + 2 * EDGE, columns), F32)
    local_scratch = [padded, padded, pltpu.VMEM((CHANNELS * PAIR, columns), F32)]
    depth_shape = pltpu.VMEM((explicit_columns.shape[1], columns), jnp.int32)

    small = [
        row_of(wet_levels),
        row_of(surface_light),
        row_of(martin_exponent),
        explicit_columns.T,
        column_slots,
    ]
    tall = pltpu.VMEM((size.levels, CHANNELS // 2, columns), F32)
    low, high, send, wet, light, exponent, column_rows, slot_rows = call(
        functools.partial(prepare_kernel, size, len(small)),
        [shape(size.low_rows), shape(size.high_rows), shape(size.send_rows, BF16)]
        + [pltpu.VMEM(value.shape, value.dtype) for value in small],
        [
            tall,
            tall,
            pltpu.VMEM((size.rows, columns), F32),
            pltpu.SemaphoreType.DMA((2 + len(small),)),
        ],
        [tracer_state.transpose(1, 0, 2), krylov_direction.transpose(1, 0, 2)] + small,
        PREPARE_FLOPS,
        tuple(range(2 + len(small))),
    )
    for time_index in range(STEPS):
        first, last = time_index == 0, time_index == STEPS - 1
        ghosts = exchange(send)
        operands = [low, high, wet, light]
        outputs = [shape(size.rows), shape(size.high_rows)]
        if first:
            partial, high, total, remineral, depth = call(
                functools.partial(local_kernel, size, "first", slots),
                outputs + [shape(1), shape(size.rows), depth_shape],
                local_scratch,
                operands + [exponent, column_rows, explicit, implicit],
                4000000,
            )
        elif last:
            partial, high, payload = call(
                functools.partial(local_kernel, size, "last", slots),
                outputs + [jax.ShapeDtypeStruct((tile_count, 1, width), F32)],
                local_scratch,
                operands + [remineral, total, explicit, implicit, slot_rows],
                4000000,
            )
            arrived = lax.all_to_all(payload, "tile", split_axis=0, concat_axis=0, tiled=True)
        else:
            partial, high, total = call(
                functools.partial(local_kernel, size, "middle", slots),
                outputs + [shape(1)],
                local_scratch,
                operands + [remineral, total, explicit, implicit],
                4000000,
            )
        operands = [partial, *ghosts, depth, wet]
        if last:
            result = jax.ShapeDtypeStruct((size.levels, CHANNELS // 2, columns), F32)
            state_out, tangent_out = call(
                functools.partial(ghost_kernel, size, True),
                [result, result],
                [
                    low_scratch,
                    pltpu.VMEM((size.rows, columns), F32),
                    tiles(2 * size.ghost_pairs),
                    tiles(2 * size.low_pairs),
                    pltpu.SemaphoreType.DMA((2,)),
                ],
                operands + [explicit_tiles, implicit_tiles, high],
                2000000,
                (6, 7),
            )
        else:
            low, send = call(
                functools.partial(ghost_kernel, size, False),
                [shape(size.low_rows), shape(size.send_rows, BF16)],
                [low_scratch],
                operands + [explicit, implicit],
            )
    (flux,) = call(
        gather_kernel, [jax.ShapeDtypeStruct((1, tile_count * slots), F32)], [], [arrived]
    )
    return state_out.transpose(1, 0, 2), tangent_out.transpose(1, 0, 2), flux.reshape(-1)


def solution(mesh):
    return jax.shard_map(
        on_device,
        mesh=mesh,
        in_specs=(
            P(None, None, ("groups", "tile")),
            P(None, None, ("groups", "tile")),
            P("tile", None, None, None),
            P("tile", None, None, None),
            P("tile", None),
            P("tile", None),
            P("tile"),
            P(("groups", "tile")),
            P(("groups", "tile")),
            P("tile", None),
        ),
        out_specs=(
            P(None, None, ("groups", "tile")),
            P(None, None, ("groups", "tile")),
            P(("groups", "tile")),
        ),
        check_vma=False,
    )
```

```python
import functools

import jax
import jax.numpy as jnp
from jax import lax
from jax.experimental import pallas as pl
from jax.experimental.pallas import tpu as pltpu
from jax.sharding import PartitionSpec as P


EUPHOTIC = 6
STEPS = 3

max_uptake = 1.0
half_saturation = 0.5
dop_fraction = 0.67
dop_decay = 0.2
time_step = 0.5

F32 = jnp.float32
BF16 = jnp.bfloat16
MIB = 1 << 20
PREPARE_FLOPS = 10**10

CHANNELS = 4
PAIR = 2 * CHANNELS
QUAD = 4 * CHANNELS
EDGE = PAIR


class Sizes:
    def __init__(self, levels, columns, depth):
        self.levels = levels
        self.columns = columns
        self.pairs = levels // 2
        self.quads = (levels + 3) // 4
        self.rows = QUAD * self.quads
        self.padded = self.rows + 2 * EDGE
        self.ghost_pairs = (depth + 1) // 2
        self.low_pairs = min((depth + 2) // 2, self.pairs)
        self.ghost_quads = (self.ghost_pairs + 1) // 2
        self.low_quads = (self.low_pairs + 1) // 2
        self.send_rows = QUAD * self.ghost_quads
        self.low_rows = PAIR * self.low_pairs
        self.high_rows = PAIR * (self.pairs - self.low_pairs)


def sublane(columns):
    return lax.broadcasted_iota(jnp.int32, (PAIR, columns), 0)


def tiles_of(ref, level, first, columns):
    return ref[level, first : first + 3].reshape(3 * columns, columns)


def pair_product(lhs, ref, pair, columns, first=0):
    rhs = jnp.concatenate(
        [tiles_of(ref, 2 * pair, first, columns), tiles_of(ref, 2 * pair + 1, first, columns)],
        axis=1,
    )
    product = jnp.dot(lhs, rhs, preferred_element_type=F32)
    top = PAIR * (pair % 2)
    upper = product[top : top + PAIR, :columns]
    lower = product[top : top + PAIR, columns:]
    return jnp.where(sublane(columns) < CHANNELS, upper, lower)


def window(ref, start, offsets):
    parts = [ref[start + offset : start + offset + QUAD, :] for offset in offsets]
    return jnp.concatenate(parts, axis=1).astype(BF16)


def wet_rows(pair, wet, columns):
    return (2 * pair + sublane(columns) // CHANNELS) < wet


def uptake_of(ref, base, wet, light, columns):
    level = lax.broadcasted_iota(jnp.int32, (PAIR, columns), 0)
    phosphate = ref[pl.ds(base, PAIR, stride=CHANNELS), :]
    direction = ref[pl.ds(base + 2, PAIR, stride=CHANNELS), :]
    scale = max_uptake * light * jnp.exp(-2.0 * level.astype(F32) / EUPHOTIC)
    scale = jnp.where((level < EUPHOTIC) & (level < wet), scale, 0.0)
    squared = phosphate * phosphate
    half = half_saturation**2
    inverse = 1.0 / (half + squared)
    uptake = scale * squared * inverse
    slope = scale * half * (2.0 * phosphate * direction) * inverse * inverse
    return uptake, slope


def passing_at(level, wet, exponent):
    ratio = (level + 1).astype(F32) / EUPHOTIC
    ratio = jnp.maximum(ratio, 1.0)
    reaching = jnp.where(level >= EUPHOTIC - 1, jnp.exp(-1.5 * exponent * jnp.log(ratio)), 1.0)
    return jnp.where(level < wet - 1, reaching, 0.0)


def prepare_kernel(size, small, *refs):
    state_hbm, krylov_hbm = refs[:2]
    small_hbm = refs[2 : 2 + small]
    low_ref, high_ref, send_ref = refs[2 + small : 5 + small]
    small_refs = refs[5 + small : 5 + 2 * small]
    state_ref, krylov_ref, fields_ref, semaphore = refs[5 + 2 * small :]
    pairs = [(state_hbm, state_ref), (krylov_hbm, krylov_ref), *zip(small_hbm, small_refs)]
    copies = [
        pltpu.make_async_copy(source, target, semaphore.at[place])
        for place, (source, target) in enumerate(pairs)
    ]
    for copy in copies:
        copy.start()
    fields_ref[...] = jnp.zeros_like(fields_ref)
    copies[0].wait()
    copies[1].wait()
    for channel in range(CHANNELS):
        source = state_ref if channel < 2 else krylov_ref
        fields_ref[pl.ds(channel, size.levels, stride=CHANNELS), :] = source[:, channel % 2, :]
    low_ref[...] = fields_ref[: size.low_rows, :]
    high_ref[...] = fields_ref[size.low_rows : size.low_rows + size.high_rows, :]
    send_ref[...] = fields_ref[: size.send_rows, :].astype(BF16)
    for copy in copies[2:]:
        copy.wait()


def local_kernel(size, stage, *refs):
    low_ref, high_ref, wet_ref, light_ref = refs[:4]
    if stage == "first":
        exponent_ref, columns_ref, explicit_ref, implicit_ref = refs[4:8]
        partial_ref, next_high_ref, total_ref, remineral_ref, depth_ref = refs[8:13]
        fields_ref, middle_ref, rate_ref = refs[13:]
    else:
        remineral_ref, explicit_ref, implicit_ref = refs[4:7]
        if stage == "middle":
            total_in_ref, partial_ref, next_high_ref, total_ref = refs[7:11]
        else:
            partial_ref, next_high_ref = refs[7:9]
        fields_ref, middle_ref, rate_ref = refs[-3:]
    columns = size.columns
    wet = wet_ref[...]
    light = light_ref[...]
    zero_edge = jnp.zeros((EDGE, columns), F32)
    live = PAIR * size.pairs
    for ref in (fields_ref, middle_ref):
        ref[:EDGE, :] = zero_edge
        for start in range(EDGE + live, size.padded, PAIR):
            ref[start : start + PAIR, :] = zero_edge
    fields_ref[EDGE : EDGE + size.low_rows, :] = low_ref[...]
    fields_ref[EDGE + size.low_rows : EDGE + live, :] = high_ref[...]
    if stage == "first":
        exponent = exponent_ref[...]
        level = lax.broadcasted_iota(jnp.int32, (size.rows // CHANNELS, columns), 0)
        above = jnp.where(level == 0, 1.0, passing_at(level - 1, wet, exponent))
        share = time_step * (above - passing_at(level, wet, exponent))
        blank = jnp.zeros_like(share)
        for channel in range(CHANNELS):
            remineral_ref[pl.ds(channel, size.rows // CHANNELS, stride=CHANNELS), :] = (
                blank if channel % 2 else share
            )
        here = (columns_ref[...] != size.levels).astype(F32)
        depth = jnp.sum(here, axis=1, keepdims=True).astype(jnp.int32)
        depth_ref[...] = jnp.broadcast_to(depth, depth_ref.shape)
    uptake, slope = uptake_of(fields_ref, EDGE, wet, light, columns)
    export = (1.0 - dop_fraction) * jnp.sum(uptake, axis=0, keepdims=True)
    export_slope = (1.0 - dop_fraction) * jnp.sum(slope, axis=0, keepdims=True)
    if stage == "first":
        total_ref[...] = export
    elif stage == "middle":
        total_ref[...] = total_in_ref[...] + export
    for channel, rate in enumerate((uptake, uptake, slope, slope)):
        factor = time_step * (dop_fraction if channel % 2 else -1.0)
        rate_ref[pl.ds(channel, PAIR, stride=CHANNELS), :] = factor * rate
    row = sublane(columns)
    sinking = jnp.where(row % CHANNELS < 2, export, export_slope)
    organic_row = row % 2 == 1

    def sources(pair):
        top = PAIR * pair
        own = fields_ref[EDGE + top : EDGE + top + PAIR, :]
        following = fields_ref[EDGE + top + 1 : EDGE + top + PAIR + 1, :]
        decayed = (time_step * dop_decay) * jnp.where(organic_row, -own, following)
        rate = jnp.where(wet_rows(pair, wet, columns), decayed, 0.0)
        rate = rate + remineral_ref[top : top + PAIR, :] * sinking
        if top < CHANNELS * PAIR:
            rate = rate + rate_ref[top : top + PAIR, :]
        return rate

    for quad in range(size.quads):
        lhs = window(fields_ref, EDGE + QUAD * quad, (0, -CHANNELS, CHANNELS))
        for pair in range(2 * quad, min(2 * quad + 2, size.pairs)):
            top = PAIR * pair
            value = pair_product(lhs, explicit_ref, pair, columns) + sources(pair)
            partial_ref[top : top + PAIR, :] = value
            middle_ref[EDGE + top : EDGE + top + PAIR, :] = value
    for start in range(live, size.rows, PAIR):
        partial_ref[start : start + PAIR, :] = zero_edge
    for quad in range(size.low_pairs // 2, size.quads):
        lhs = window(middle_ref, EDGE + QUAD * quad, (-CHANNELS, 0, CHANNELS))
        for pair in range(max(2 * quad, size.low_pairs), min(2 * quad + 2, size.pairs)):
            settled = pair_product(lhs, implicit_ref, pair, columns)
            top = PAIR * (pair - size.low_pairs)
            next_high_ref[top : top + PAIR, :] = jnp.where(
                wet_rows(pair, wet, columns), settled, 0.0
            )


def place_slots(total, slots_ref, slots, width):
    targets = slots_ref.shape[0]
    column = lax.broadcasted_iota(jnp.int32, (targets, total.shape[1]), 1)
    lane = lax.broadcasted_iota(jnp.int32, (targets, width), 1) - slots * lax.axis_index("tile")
    placed = jnp.zeros((targets, width), F32)
    for slot in range(slots):
        chosen = column == slots_ref[:, slot : slot + 1]
        value = jnp.sum(jnp.where(chosen, total, 0.0), axis=1, keepdims=True)
        placed = jnp.where(lane == slot, value, placed)
    return placed


def halves(rows):
    half = rows.shape[0] // 2
    upper = (lax.axis_index("tile") // half) % 2 == 1
    first, second = rows[:half], rows[half:]
    return jnp.where(upper, second, first), jnp.where(upper, first, second)


def route_kernel(packed, *refs):
    kept_ref, arrived_ref, keep_ref, send_ref = refs
    rows = kept_ref[...]
    if packed:
        count, width = rows.shape
        base = arrived_ref.shape[0] - 2 * count * (width // 128)
        parts = [
            arrived_ref[base + count * k : base + count * (k + 1), :].astype(F32)
            for k in range(2 * (width // 128))
        ]
        high = jnp.concatenate(parts[: width // 128], axis=1)
        low = jnp.concatenate(parts[width // 128 :], axis=1)
        rows = rows + (high + low)
    else:
        rows = rows + arrived_ref[...]
    keep_ref[...], send_ref[...] = halves(rows)


def flux_kernel(kept_ref, arrived_ref, flux_ref):
    flux = kept_ref[...] + arrived_ref[...]
    flux_ref[...] = flux[:, : flux_ref.shape[1]]


def ghost_kernel(size, stage, slots, *refs):
    partial_ref, pair_ref, other_ref, across_ref, depth_ref, wet_ref, explicit_ref, implicit_ref = refs[:8]
    if stage == "last":
        high_ref, state_ref, tangent_ref, middle_ref, fields_ref = refs[8:]
    elif stage == "export":
        light_ref, total_ref, slots_ref, low_ref, send_ref, across_out_ref, keep_ref, middle_ref = refs[8:]
    else:
        low_ref, send_ref, middle_ref = refs[8:]
    columns = size.columns
    wet = wet_ref[...]
    even = lax.axis_index("tile") % 2 == 0
    middle_ref[:EDGE, :] = jnp.zeros((EDGE, columns), F32)
    for top in range(PAIR * size.ghost_pairs, QUAD * size.low_quads + EDGE, PAIR):
        middle_ref[EDGE + top : EDGE + top + PAIR, :] = partial_ref[top : top + PAIR, :]
    for quad in range(size.ghost_quads):
        span = slice(QUAD * quad, QUAD * quad + QUAD)
        own_chip = pair_ref[span, :].astype(F32)
        next_chip = other_ref[span, :].astype(F32)
        across = across_ref[span, :].astype(F32)
        level = lax.broadcasted_iota(jnp.int32, (QUAD, columns), 0) // CHANNELS + CHANNELS * quad
        before = jnp.where(even, next_chip, own_chip)
        after = jnp.where(even, own_chip, next_chip)
        before = jnp.where(level < depth_ref[3:4, :], before, 0.0)
        after = jnp.where(level < depth_ref[4:5, :], after, 0.0)
        across = jnp.where(level < depth_ref[5:6, :], across, 0.0)
        lhs = jnp.concatenate([before, after, across], axis=1).astype(BF16)
        for pair in range(2 * quad, min(2 * quad + 2, size.ghost_pairs)):
            top = PAIR * pair
            value = pair_product(lhs, explicit_ref, pair, columns, 3)
            middle_ref[EDGE + top : EDGE + top + PAIR, :] = value + partial_ref[top : top + PAIR, :]
    values = []
    for quad in range(size.low_quads):
        lhs = window(middle_ref, EDGE + QUAD * quad, (-CHANNELS, 0, CHANNELS))
        for pair in range(2 * quad, min(2 * quad + 2, size.low_pairs)):
            settled = pair_product(lhs, implicit_ref, pair, columns)
            values.append(jnp.where(wet_rows(pair, wet, columns), settled, 0.0))
    if stage == "last":
        for pair, value in enumerate(values):
            fields_ref[PAIR * pair : PAIR * pair + PAIR, :] = value
        fields_ref[size.low_rows : size.low_rows + size.high_rows, :] = high_ref[...]
        for channel in range(CHANNELS):
            out_ref = state_ref if channel < 2 else tangent_ref
            out_ref[:, channel % 2, :] = fields_ref[pl.ds(channel, size.levels, stride=CHANNELS), :]
        return
    for pair, value in enumerate(values):
        low_ref[PAIR * pair : PAIR * pair + PAIR, :] = value
    blank = jnp.zeros((PAIR, columns), F32)
    for quad in range(size.ghost_quads):
        two = [
            values[pair] if pair < len(values) else blank for pair in (2 * quad, 2 * quad + 1)
        ]
        rows = jnp.concatenate(two, axis=0).astype(BF16)
        send_ref[QUAD * quad : QUAD * quad + QUAD, :] = rows
        if stage == "export":
            across_out_ref[QUAD * quad : QUAD * quad + QUAD, :] = rows
    if stage == "export":
        uptake, _ = uptake_of(low_ref, 0, wet, light_ref[...], columns)
        total = total_ref[...] + (1.0 - dop_fraction) * jnp.sum(uptake, axis=0, keepdims=True)
        placed = place_slots(total, slots_ref, slots, keep_ref.shape[1])
        keep_ref[...], leaving = halves(placed)
        width = leaving.shape[1]
        high = leaving.astype(BF16).astype(F32)
        parts = [
            part[:, start : start + 128]
            for part in (high, leaving - high)
            for start in range(0, width, 128)
        ]
        across_out_ref[size.send_rows :, :] = jnp.concatenate(parts, axis=0).astype(BF16)


def in_vmem(value):
    return pltpu.with_memory_space_constraint(value, pltpu.VMEM)


def call(body, outputs, scratch, operands, flops=1000000, in_hbm=()):
    space = lambda place: pltpu.HBM if place in in_hbm else pltpu.VMEM
    operands = [
        pltpu.with_memory_space_constraint(value, pltpu.HBM) if place in in_hbm else value
        for place, value in enumerate(operands)
    ]
    return pl.pallas_call(
        body,
        out_shape=outputs,
        in_specs=[pl.BlockSpec(memory_space=space(k)) for k in range(len(operands))],
        out_specs=[pl.BlockSpec(memory_space=pltpu.VMEM)] * len(outputs),
        scratch_shapes=scratch,
        compiler_params=pltpu.CompilerParams(vmem_limit_bytes=8 * MIB),
        cost_estimate=pl.CostEstimate(flops=flops, bytes_accessed=100000, transcendentals=0),
    )(*operands)


def on_device(
    tracer_state,
    krylov_direction,
    explicit_tiles,
    implicit_tiles,
    explicit_columns,
    ghost_levels,
    wet_levels,
    surface_light,
    martin_exponent,
    column_slots,
):
    size = Sizes(tracer_state.shape[1], tracer_state.shape[2], ghost_levels.shape[1])
    columns = size.columns
    tile_count = lax.axis_size("tile")
    assert tile_count & (tile_count - 1) == 0
    slots = column_slots.shape[1]
    width = -(-tile_count * slots // 128) * 128
    row_of = lambda value: value.reshape(1, columns)
    explicit, implicit = in_vmem(explicit_tiles), in_vmem(implicit_tiles)

    same_chip = [(d, d ^ 1) for d in range(tile_count)]
    next_chip = [(d, (d + (1 if d % 2 else -1)) % tile_count) for d in range(tile_count)]
    opposite = [(d, (d + tile_count // 2) % tile_count) for d in range(tile_count)]

    def exchange(value, across_value):
        across = lax.ppermute(across_value, "tile", opposite)
        other = lax.ppermute(value, "tile", next_chip)
        pair = lax.ppermute(value, "tile", same_chip)
        return pair, other, across

    def shape(rows, dtype=F32):
        return pltpu.VMEM((rows, columns), dtype)

    padded = pltpu.VMEM((size.padded, columns), F32)
    low_scratch = pltpu.VMEM((QUAD * size.low_quads + 2 * EDGE, columns), F32)
    local_scratch = [padded, padded, pltpu.VMEM((CHANNELS * PAIR, columns), F32)]
    depth_shape = pltpu.VMEM((explicit_columns.shape[1], columns), jnp.int32)

    small = [
        row_of(wet_levels),
        row_of(surface_light),
        row_of(martin_exponent),
        explicit_columns.T,
        column_slots,
    ]
    tall = pltpu.VMEM((size.levels, CHANNELS // 2, columns), F32)
    low, high, send, wet, light, exponent, column_rows, slot_rows = call(
        functools.partial(prepare_kernel, size, len(small)),
        [shape(size.low_rows), shape(size.high_rows), shape(size.send_rows, BF16)]
        + [pltpu.VMEM(value.shape, value.dtype) for value in small],
        [
            tall,
            tall,
            pltpu.VMEM((size.rows, columns), F32),
            pltpu.SemaphoreType.DMA((2 + len(small),)),
        ],
        [tracer_state.transpose(1, 0, 2), krylov_direction.transpose(1, 0, 2)] + small,
        PREPARE_FLOPS,
        tuple(range(2 + len(small))),
    )
    across_send = send
    for time_index in range(STEPS):
        first, last = time_index == 0, time_index == STEPS - 1
        ghosts = exchange(send, across_send)
        operands = [low, high, wet, light]
        outputs = [shape(size.rows), shape(size.high_rows)]
        weights = [explicit, implicit]
        if first:
            partial, high, total, remineral, depth = call(
                functools.partial(local_kernel, size, "first"),
                outputs + [shape(1), shape(size.rows), depth_shape],
                local_scratch,
                operands + [exponent, column_rows] + weights,
                4000000,
            )
        elif last:
            partial, high = call(
                functools.partial(local_kernel, size, "last"),
                outputs,
                local_scratch,
                operands + [remineral] + weights,
                4000000,
            )
        else:
            partial, high, total = call(
                functools.partial(local_kernel, size, "middle"),
                outputs + [shape(1)],
                local_scratch,
                operands + [remineral] + weights + [total],
                4000000,
            )
        operands = [partial, *ghosts, depth, wet] + weights
        sends = [shape(size.low_rows), shape(size.send_rows, BF16)]
        if last:
            result = jax.ShapeDtypeStruct((size.levels, CHANNELS // 2, columns), F32)
            state_out, tangent_out = call(
                functools.partial(ghost_kernel, size, "last", slots),
                [result, result],
                [low_scratch, pltpu.VMEM((size.rows, columns), F32)],
                operands + [high],
                2000000,
            )
        elif time_index == STEPS - 2:
            half = tile_count // 2
            packed_rows = size.send_rows + 2 * half * (width // 128)
            low, send, across_send, kept = call(
                functools.partial(ghost_kernel, size, "export", slots),
                sends + [shape(packed_rows, BF16), pltpu.VMEM((half, width), F32)],
                [low_scratch],
                operands + [light, total, slot_rows],
            )
        else:
            low, send = call(
                functools.partial(ghost_kernel, size, "middle", slots),
                sends,
                [low_scratch],
                operands,
            )
            across_send = send
    arrived, half = ghosts[2], tile_count // 2
    while half > 1:
        half //= 2
        piece = pltpu.VMEM((half, width), F32)
        kept, leaving = call(
            functools.partial(route_kernel, 2 * half == tile_count // 2),
            [piece, piece],
            [],
            [kept, arrived],
        )
        partners = [(d, d ^ half) for d in range(tile_count)]
        arrived = lax.ppermute(leaving, "tile", partners)
    (flux,) = call(
        flux_kernel, [jax.ShapeDtypeStruct((1, tile_count * slots), F32)], [], [kept, arrived]
    )
    return state_out.transpose(1, 0, 2), tangent_out.transpose(1, 0, 2), flux.reshape(-1)


def solution(mesh):
    return jax.shard_map(
        on_device,
        mesh=mesh,
        in_specs=(
            P(None, None, ("groups", "tile")),
            P(None, None, ("groups", "tile")),
            P("tile", None, None, None),
            P("tile", None, None, None),
            P("tile", None),
            P("tile", None),
            P("tile"),
            P(("groups", "tile")),
            P(("groups", "tile")),
            P("tile", None),
        ),
        out_specs=(
            P(None, None, ("groups", "tile")),
            P(None, None, ("groups", "tile")),
            P(("groups", "tile")),
        ),
        check_vma=False,
    )
```

```python
import functools

import jax
import jax.numpy as jnp
from jax import lax
from jax.experimental import pallas as pl
from jax.experimental.pallas import tpu as pltpu
from jax.sharding import PartitionSpec as P


EUPHOTIC = 6
STEPS = 3

max_uptake = 1.0
half_saturation = 0.5
dop_fraction = 0.67
dop_decay = 0.2
time_step = 0.5

F32 = jnp.float32
BF16 = jnp.bfloat16
MIB = 1 << 20
PREPARE_FLOPS = 10**10

CHANNELS = 4
PAIR = 2 * CHANNELS
QUAD = 4 * CHANNELS
EDGE = PAIR


class Sizes:
    def __init__(self, levels, columns, depth):
        self.levels = levels
        self.columns = columns
        self.pairs = levels // 2
        self.quads = (levels + 3) // 4
        self.rows = QUAD * self.quads
        self.padded = self.rows + 2 * EDGE
        self.ghost_pairs = (depth + 1) // 2
        self.low_pairs = min((depth + 2) // 2, self.pairs)
        self.ghost_quads = (self.ghost_pairs + 1) // 2
        self.low_quads = (self.low_pairs + 1) // 2
        self.send_rows = QUAD * self.ghost_quads
        self.low_rows = PAIR * self.low_pairs
        self.high_rows = PAIR * (self.pairs - self.low_pairs)


def sublane(columns):
    return lax.broadcasted_iota(jnp.int32, (PAIR, columns), 0)


def tiles_of(ref, level, first, columns):
    return ref[level, first : first + 3].reshape(3 * columns, columns)


def pair_product(lhs, ref, pair, columns, first=0):
    rhs = jnp.concatenate(
        [tiles_of(ref, 2 * pair, first, columns), tiles_of(ref, 2 * pair + 1, first, columns)],
        axis=1,
    )
    product = jnp.dot(lhs, rhs, preferred_element_type=F32)
    top = PAIR * (pair % 2)
    upper = product[top : top + PAIR, :columns]
    lower = product[top : top + PAIR, columns:]
    return jnp.where(sublane(columns) < CHANNELS, upper, lower)


def window(ref, start, offsets):
    parts = [ref[start + offset : start + offset + QUAD, :] for offset in offsets]
    return jnp.concatenate(parts, axis=1).astype(BF16)


def wet_rows(pair, wet, columns):
    return (2 * pair + sublane(columns) // CHANNELS) < wet


def uptake_of(ref, base, wet, light, columns):
    level = lax.broadcasted_iota(jnp.int32, (PAIR, columns), 0)
    phosphate = ref[pl.ds(base, PAIR, stride=CHANNELS), :]
    direction = ref[pl.ds(base + 2, PAIR, stride=CHANNELS), :]
    scale = max_uptake * light * jnp.exp(-2.0 * level.astype(F32) / EUPHOTIC)
    scale = jnp.where((level < EUPHOTIC) & (level < wet), scale, 0.0)
    squared = phosphate * phosphate
    half = half_saturation**2
    inverse = 1.0 / (half + squared)
    uptake = scale * squared * inverse
    slope = scale * half * (2.0 * phosphate * direction) * inverse * inverse
    return uptake, slope


def passing_at(level, wet, exponent):
    ratio = (level + 1).astype(F32) / EUPHOTIC
    ratio = jnp.maximum(ratio, 1.0)
    reaching = jnp.where(level >= EUPHOTIC - 1, jnp.exp(-1.5 * exponent * jnp.log(ratio)), 1.0)
    return jnp.where(level < wet - 1, reaching, 0.0)


def prepare_kernel(size, small, *refs):
    state_hbm, krylov_hbm = refs[:2]
    small_hbm = refs[2 : 2 + small]
    low_ref, high_ref, send_ref = refs[2 + small : 5 + small]
    small_refs = refs[5 + small : 5 + 2 * small]
    state_ref, krylov_ref, fields_ref, semaphore = refs[5 + 2 * small :]
    pairs = [(state_hbm, state_ref), (krylov_hbm, krylov_ref), *zip(small_hbm, small_refs)]
    copies = [
        pltpu.make_async_copy(source, target, semaphore.at[place])
        for place, (source, target) in enumerate(pairs)
    ]
    for copy in copies:
        copy.start()
    fields_ref[...] = jnp.zeros_like(fields_ref)
    copies[0].wait()
    copies[1].wait()
    for channel in range(CHANNELS):
        source = state_ref if channel < 2 else krylov_ref
        fields_ref[pl.ds(channel, size.levels, stride=CHANNELS), :] = source[:, channel % 2, :]
    low_ref[...] = fields_ref[: size.low_rows, :]
    high_ref[...] = fields_ref[size.low_rows : size.low_rows + size.high_rows, :]
    send_ref[...] = fields_ref[: size.send_rows, :].astype(BF16)
    for copy in copies[2:]:
        copy.wait()


def local_kernel(size, stage, *refs):
    low_ref, high_ref, wet_ref, light_ref = refs[:4]
    if stage == "first":
        exponent_ref, columns_ref, explicit_ref, implicit_ref = refs[4:8]
        partial_ref, next_high_ref, total_ref, remineral_ref, depth_ref = refs[8:13]
        fields_ref, middle_ref, rate_ref = refs[13:]
    else:
        remineral_ref, explicit_ref, implicit_ref = refs[4:7]
        if stage == "middle":
            total_in_ref, partial_ref, next_high_ref, total_ref = refs[7:11]
        else:
            partial_ref, next_high_ref = refs[7:9]
        fields_ref, middle_ref, rate_ref = refs[-3:]
    columns = size.columns
    wet = wet_ref[...]
    light = light_ref[...]
    zero_edge = jnp.zeros((EDGE, columns), F32)
    live = PAIR * size.pairs
    for ref in (fields_ref, middle_ref):
        ref[:EDGE, :] = zero_edge
        for start in range(EDGE + live, size.padded, PAIR):
            ref[start : start + PAIR, :] = zero_edge
    fields_ref[EDGE : EDGE + size.low_rows, :] = low_ref[...]
    fields_ref[EDGE + size.low_rows : EDGE + live, :] = high_ref[...]
    if stage == "first":
        exponent = exponent_ref[...]
        level = lax.broadcasted_iota(jnp.int32, (size.rows // CHANNELS, columns), 0)
        above = jnp.where(level == 0, 1.0, passing_at(level - 1, wet, exponent))
        share = time_step * (above - passing_at(level, wet, exponent))
        blank = jnp.zeros_like(share)
        for channel in range(CHANNELS):
            remineral_ref[pl.ds(channel, size.rows // CHANNELS, stride=CHANNELS), :] = (
                blank if channel % 2 else share
            )
        here = (columns_ref[...] != size.levels).astype(F32)
        depth = jnp.sum(here, axis=1, keepdims=True).astype(jnp.int32)
        depth_ref[...] = jnp.broadcast_to(depth, depth_ref.shape)
    uptake, slope = uptake_of(fields_ref, EDGE, wet, light, columns)
    export = (1.0 - dop_fraction) * jnp.sum(uptake, axis=0, keepdims=True)
    export_slope = (1.0 - dop_fraction) * jnp.sum(slope, axis=0, keepdims=True)
    if stage == "first":
        total_ref[...] = export
    elif stage == "middle":
        total_ref[...] = total_in_ref[...] + export
    for channel, rate in enumerate((uptake, uptake, slope, slope)):
        factor = time_step * (dop_fraction if channel % 2 else -1.0)
        rate_ref[pl.ds(channel, PAIR, stride=CHANNELS), :] = factor * rate
    row = sublane(columns)
    sinking = jnp.where(row % CHANNELS < 2, export, export_slope)
    organic_row = row % 2 == 1

    def sources(pair):
        top = PAIR * pair
        own = fields_ref[EDGE + top : EDGE + top + PAIR, :]
        following = fields_ref[EDGE + top + 1 : EDGE + top + PAIR + 1, :]
        decayed = (time_step * dop_decay) * jnp.where(organic_row, -own, following)
        rate = jnp.where(wet_rows(pair, wet, columns), decayed, 0.0)
        rate = rate + remineral_ref[top : top + PAIR, :] * sinking
        if top < CHANNELS * PAIR:
            rate = rate + rate_ref[top : top + PAIR, :]
        return rate

    for quad in range(size.quads):
        lhs = window(fields_ref, EDGE + QUAD * quad, (0, -CHANNELS, CHANNELS))
        for pair in range(2 * quad, min(2 * quad + 2, size.pairs)):
            top = PAIR * pair
            value = pair_product(lhs, explicit_ref, pair, columns) + sources(pair)
            partial_ref[top : top + PAIR, :] = value
            middle_ref[EDGE + top : EDGE + top + PAIR, :] = value
    for start in range(live, size.rows, PAIR):
        partial_ref[start : start + PAIR, :] = zero_edge
    for quad in range(size.low_pairs // 2, size.quads):
        lhs = window(middle_ref, EDGE + QUAD * quad, (-CHANNELS, 0, CHANNELS))
        for pair in range(max(2 * quad, size.low_pairs), min(2 * quad + 2, size.pairs)):
            settled = pair_product(lhs, implicit_ref, pair, columns)
            top = PAIR * (pair - size.low_pairs)
            next_high_ref[top : top + PAIR, :] = jnp.where(
                wet_rows(pair, wet, columns), settled, 0.0
            )


def place_slots(total, slots_ref, slots, width):
    targets = slots_ref.shape[0]
    column = lax.broadcasted_iota(jnp.int32, (targets, total.shape[1]), 1)
    lane = lax.broadcasted_iota(jnp.int32, (targets, width), 1) - slots * lax.axis_index("tile")
    placed = jnp.zeros((targets, width), F32)
    for slot in range(slots):
        chosen = column == slots_ref[:, slot : slot + 1]
        value = jnp.sum(jnp.where(chosen, total, 0.0), axis=1, keepdims=True)
        placed = jnp.where(lane == slot, value, placed)
    return placed


def halves(rows):
    half = rows.shape[0] // 2
    upper = (lax.axis_index("tile") // half) % 2 == 1
    first, second = rows[:half], rows[half:]
    return jnp.where(upper, second, first), jnp.where(upper, first, second)


def route_kernel(packed, *refs):
    kept_ref, arrived_ref, keep_ref, *send_refs = refs
    rows = kept_ref[...]
    if packed:
        count, width = rows.shape
        base = arrived_ref.shape[0] - 2 * count * (width // 128)
        parts = [
            arrived_ref[base + count * k : base + count * (k + 1), :].astype(F32)
            for k in range(2 * (width // 128))
        ]
        high = jnp.concatenate(parts[: width // 128], axis=1)
        low = jnp.concatenate(parts[width // 128 :], axis=1)
        rows = rows + (high + low)
    else:
        rows = rows + arrived_ref[...]
    mine, other = halves(rows)
    if len(send_refs) == 1:
        keep_ref[...], send_refs[0][...] = mine, other
    else:
        keep_ref[...], send_refs[0][...] = halves(mine)
        send_refs[1][...], send_refs[2][...] = halves(other)


def flux_kernel(*refs):
    *part_refs, flux_ref = refs
    flux = part_refs[0][...]
    for ref in part_refs[1:]:
        flux = flux + ref[...]
    flux_ref[...] = flux[:, : flux_ref.shape[1]]


def ghost_kernel(size, stage, slots, *refs):
    partial_ref, pair_ref, other_ref, across_ref, depth_ref, wet_ref, explicit_ref, implicit_ref = refs[:8]
    if stage == "last":
        high_ref, state_ref, tangent_ref, middle_ref, fields_ref = refs[8:]
    elif stage == "export":
        light_ref, total_ref, slots_ref, low_ref, send_ref, across_out_ref, keep_ref, middle_ref = refs[8:]
    else:
        low_ref, send_ref, middle_ref = refs[8:]
    columns = size.columns
    wet = wet_ref[...]
    even = lax.axis_index("tile") % 2 == 0
    middle_ref[:EDGE, :] = jnp.zeros((EDGE, columns), F32)
    for top in range(PAIR * size.ghost_pairs, QUAD * size.low_quads + EDGE, PAIR):
        middle_ref[EDGE + top : EDGE + top + PAIR, :] = partial_ref[top : top + PAIR, :]
    for quad in range(size.ghost_quads):
        span = slice(QUAD * quad, QUAD * quad + QUAD)
        own_chip = pair_ref[span, :].astype(F32)
        next_chip = other_ref[span, :].astype(F32)
        across = across_ref[span, :].astype(F32)
        level = lax.broadcasted_iota(jnp.int32, (QUAD, columns), 0) // CHANNELS + CHANNELS * quad
        before = jnp.where(even, next_chip, own_chip)
        after = jnp.where(even, own_chip, next_chip)
        before = jnp.where(level < depth_ref[3:4, :], before, 0.0)
        after = jnp.where(level < depth_ref[4:5, :], after, 0.0)
        across = jnp.where(level < depth_ref[5:6, :], across, 0.0)
        lhs = jnp.concatenate([before, after, across], axis=1).astype(BF16)
        for pair in range(2 * quad, min(2 * quad + 2, size.ghost_pairs)):
            top = PAIR * pair
            value = pair_product(lhs, explicit_ref, pair, columns, 3)
            middle_ref[EDGE + top : EDGE + top + PAIR, :] = value + partial_ref[top : top + PAIR, :]
    values = []
    for quad in range(size.low_quads):
        lhs = window(middle_ref, EDGE + QUAD * quad, (-CHANNELS, 0, CHANNELS))
        for pair in range(2 * quad, min(2 * quad + 2, size.low_pairs)):
            settled = pair_product(lhs, implicit_ref, pair, columns)
            values.append(jnp.where(wet_rows(pair, wet, columns), settled, 0.0))
    if stage == "last":
        for pair, value in enumerate(values):
            fields_ref[PAIR * pair : PAIR * pair + PAIR, :] = value
        fields_ref[size.low_rows : size.low_rows + size.high_rows, :] = high_ref[...]
        for channel in range(CHANNELS):
            out_ref = state_ref if channel < 2 else tangent_ref
            out_ref[:, channel % 2, :] = fields_ref[pl.ds(channel, size.levels, stride=CHANNELS), :]
        return
    for pair, value in enumerate(values):
        low_ref[PAIR * pair : PAIR * pair + PAIR, :] = value
    blank = jnp.zeros((PAIR, columns), F32)
    for quad in range(size.ghost_quads):
        two = [
            values[pair] if pair < len(values) else blank for pair in (2 * quad, 2 * quad + 1)
        ]
        rows = jnp.concatenate(two, axis=0).astype(BF16)
        send_ref[QUAD * quad : QUAD * quad + QUAD, :] = rows
        if stage == "export":
            across_out_ref[QUAD * quad : QUAD * quad + QUAD, :] = rows
    if stage == "export":
        uptake, _ = uptake_of(low_ref, 0, wet, light_ref[...], columns)
        total = total_ref[...] + (1.0 - dop_fraction) * jnp.sum(uptake, axis=0, keepdims=True)
        placed = place_slots(total, slots_ref, slots, keep_ref.shape[1])
        keep_ref[...], leaving = halves(placed)
        width = leaving.shape[1]
        high = leaving.astype(BF16).astype(F32)
        parts = [
            part[:, start : start + 128]
            for part in (high, leaving - high)
            for start in range(0, width, 128)
        ]
        across_out_ref[size.send_rows :, :] = jnp.concatenate(parts, axis=0).astype(BF16)


def in_vmem(value):
    return pltpu.with_memory_space_constraint(value, pltpu.VMEM)


def call(body, outputs, scratch, operands, flops=1000000, in_hbm=()):
    space = lambda place: pltpu.HBM if place in in_hbm else pltpu.VMEM
    operands = [
        pltpu.with_memory_space_constraint(value, pltpu.HBM) if place in in_hbm else value
        for place, value in enumerate(operands)
    ]
    return pl.pallas_call(
        body,
        out_shape=outputs,
        in_specs=[pl.BlockSpec(memory_space=space(k)) for k in range(len(operands))],
        out_specs=[pl.BlockSpec(memory_space=pltpu.VMEM)] * len(outputs),
        scratch_shapes=scratch,
        compiler_params=pltpu.CompilerParams(vmem_limit_bytes=8 * MIB),
        cost_estimate=pl.CostEstimate(flops=flops, bytes_accessed=100000, transcendentals=0),
    )(*operands)


def on_device(
    tracer_state,
    krylov_direction,
    explicit_tiles,
    implicit_tiles,
    explicit_columns,
    ghost_levels,
    wet_levels,
    surface_light,
    martin_exponent,
    column_slots,
):
    size = Sizes(tracer_state.shape[1], tracer_state.shape[2], ghost_levels.shape[1])
    columns = size.columns
    tile_count = lax.axis_size("tile")
    assert tile_count & (tile_count - 1) == 0
    slots = column_slots.shape[1]
    width = -(-tile_count * slots // 128) * 128
    row_of = lambda value: value.reshape(1, columns)
    explicit, implicit = in_vmem(explicit_tiles), in_vmem(implicit_tiles)

    same_chip = [(d, d ^ 1) for d in range(tile_count)]
    next_chip = [(d, (d + (1 if d % 2 else -1)) % tile_count) for d in range(tile_count)]
    opposite = [(d, (d + tile_count // 2) % tile_count) for d in range(tile_count)]

    def exchange(value, across_value):
        across = lax.ppermute(across_value, "tile", opposite)
        other = lax.ppermute(value, "tile", next_chip)
        pair = lax.ppermute(value, "tile", same_chip)
        return pair, other, across

    def shape(rows, dtype=F32):
        return pltpu.VMEM((rows, columns), dtype)

    padded = pltpu.VMEM((size.padded, columns), F32)
    low_scratch = pltpu.VMEM((QUAD * size.low_quads + 2 * EDGE, columns), F32)
    local_scratch = [padded, padded, pltpu.VMEM((CHANNELS * PAIR, columns), F32)]
    depth_shape = pltpu.VMEM((explicit_columns.shape[1], columns), jnp.int32)

    small = [
        row_of(wet_levels),
        row_of(surface_light),
        row_of(martin_exponent),
        explicit_columns.T,
        column_slots,
    ]
    tall = pltpu.VMEM((size.levels, CHANNELS // 2, columns), F32)
    low, high, send, wet, light, exponent, column_rows, slot_rows = call(
        functools.partial(prepare_kernel, size, len(small)),
        [shape(size.low_rows), shape(size.high_rows), shape(size.send_rows, BF16)]
        + [pltpu.VMEM(value.shape, value.dtype) for value in small],
        [
            tall,
            tall,
            pltpu.VMEM((size.rows, columns), F32),
            pltpu.SemaphoreType.DMA((2 + len(small),)),
        ],
        [tracer_state.transpose(1, 0, 2), krylov_direction.transpose(1, 0, 2)] + small,
        PREPARE_FLOPS,
        tuple(range(2 + len(small))),
    )
    across_send = send
    for time_index in range(STEPS):
        first, last = time_index == 0, time_index == STEPS - 1
        ghosts = exchange(send, across_send)
        operands = [low, high, wet, light]
        outputs = [shape(size.rows), shape(size.high_rows)]
        weights = [explicit, implicit]
        if first:
            partial, high, total, remineral, depth = call(
                functools.partial(local_kernel, size, "first"),
                outputs + [shape(1), shape(size.rows), depth_shape],
                local_scratch,
                operands + [exponent, column_rows] + weights,
                4000000,
            )
        elif last:
            partial, high = call(
                functools.partial(local_kernel, size, "last"),
                outputs,
                local_scratch,
                operands + [remineral] + weights,
                4000000,
            )
        else:
            partial, high, total = call(
                functools.partial(local_kernel, size, "middle"),
                outputs + [shape(1)],
                local_scratch,
                operands + [remineral] + weights + [total],
                4000000,
            )
        operands = [partial, *ghosts, depth, wet] + weights
        sends = [shape(size.low_rows), shape(size.send_rows, BF16)]
        if last:
            result = jax.ShapeDtypeStruct((size.levels, CHANNELS // 2, columns), F32)
            state_out, tangent_out = call(
                functools.partial(ghost_kernel, size, "last", slots),
                [result, result],
                [low_scratch, pltpu.VMEM((size.rows, columns), F32)],
                operands + [high],
                2000000,
            )
        elif time_index == STEPS - 2:
            half = tile_count // 2
            packed_rows = size.send_rows + 2 * half * (width // 128)
            low, send, across_send, kept = call(
                functools.partial(ghost_kernel, size, "export", slots),
                sends + [shape(packed_rows, BF16), pltpu.VMEM((half, width), F32)],
                [low_scratch],
                operands + [light, total, slot_rows],
            )
        else:
            low, send = call(
                functools.partial(ghost_kernel, size, "middle", slots),
                sends,
                [low_scratch],
                operands,
            )
            across_send = send
    arrived, half = ghosts[2], tile_count // 2
    while half > 1:
        packed = 2 * half == tile_count
        step = 4 if half == 4 else 2
        half //= step
        piece = pltpu.VMEM((half, width), F32)
        kept, *leaving = call(
            functools.partial(route_kernel, packed), [piece] * step, [], [kept, arrived]
        )
        pieces = []
        for place, value in enumerate(leaving, 1):
            away = place * half
            partners = [(d, d ^ away) for d in range(tile_count)]
            pieces.append(lax.ppermute(value, "tile", partners))
        arrived = pieces[0]
    (flux,) = call(
        flux_kernel, [jax.ShapeDtypeStruct((1, tile_count * slots), F32)], [], [kept, *pieces]
    )
    return state_out.transpose(1, 0, 2), tangent_out.transpose(1, 0, 2), flux.reshape(-1)


def solution(mesh):
    return jax.shard_map(
        on_device,
        mesh=mesh,
        in_specs=(
            P(None, None, ("groups", "tile")),
            P(None, None, ("groups", "tile")),
            P("tile", None, None, None),
            P("tile", None, None, None),
            P("tile", None),
            P("tile", None),
            P("tile"),
            P(("groups", "tile")),
            P(("groups", "tile")),
            P("tile", None),
        ),
        out_specs=(
            P(None, None, ("groups", "tile")),
            P(None, None, ("groups", "tile")),
            P(("groups", "tile")),
        ),
        check_vma=False,
    )
```

```python
import functools

import jax
import jax.numpy as jnp
from jax import lax
from jax.experimental import pallas as pl
from jax.experimental.pallas import tpu as pltpu
from jax.sharding import PartitionSpec as P


EUPHOTIC = 6
STEPS = 3

max_uptake = 1.0
half_saturation = 0.5
dop_fraction = 0.67
dop_decay = 0.2
time_step = 0.5

F32 = jnp.float32
BF16 = jnp.bfloat16
MIB = 1 << 20
PREPARE_FLOPS = 10**10

CHANNELS = 4
PAIR = 2 * CHANNELS
QUAD = 4 * CHANNELS
EDGE = PAIR


class Sizes:
    def __init__(self, levels, columns, depth):
        self.levels = levels
        self.columns = columns
        self.pairs = levels // 2
        self.quads = (levels + 3) // 4
        self.rows = QUAD * self.quads
        self.padded = self.rows + 2 * EDGE
        self.ghost_pairs = (depth + 1) // 2
        self.low_pairs = min((depth + 2) // 2, self.pairs)
        self.ghost_quads = (self.ghost_pairs + 1) // 2
        self.low_quads = (self.low_pairs + 1) // 2
        self.send_rows = QUAD * self.ghost_quads
        self.low_rows = PAIR * self.low_pairs
        self.high_rows = PAIR * (self.pairs - self.low_pairs)


def sublane(columns):
    return lax.broadcasted_iota(jnp.int32, (PAIR, columns), 0)


def tiles_of(ref, level, first, columns):
    return ref[level, first : first + 3].reshape(3 * columns, columns)


def pair_product(lhs, ref, pair, columns, first=0):
    rhs = jnp.concatenate(
        [tiles_of(ref, 2 * pair, first, columns), tiles_of(ref, 2 * pair + 1, first, columns)],
        axis=1,
    )
    product = jnp.dot(lhs, rhs, preferred_element_type=F32)
    top = PAIR * (pair % 2)
    upper = product[top : top + PAIR, :columns]
    lower = product[top : top + PAIR, columns:]
    return jnp.where(sublane(columns) < CHANNELS, upper, lower)


def window(ref, start, offsets):
    parts = [ref[start + offset : start + offset + QUAD, :] for offset in offsets]
    return jnp.concatenate(parts, axis=1).astype(BF16)


def wet_rows(pair, wet, columns):
    return (2 * pair + sublane(columns) // CHANNELS) < wet


def uptake_of(ref, base, wet, light, columns):
    level = lax.broadcasted_iota(jnp.int32, (PAIR, columns), 0)
    phosphate = ref[pl.ds(base, PAIR, stride=CHANNELS), :]
    direction = ref[pl.ds(base + 2, PAIR, stride=CHANNELS), :]
    scale = max_uptake * light * jnp.exp(-2.0 * level.astype(F32) / EUPHOTIC)
    scale = jnp.where((level < EUPHOTIC) & (level < wet), scale, 0.0)
    squared = phosphate * phosphate
    half = half_saturation**2
    inverse = 1.0 / (half + squared)
    uptake = scale * squared * inverse
    slope = scale * half * (2.0 * phosphate * direction) * inverse * inverse
    return uptake, slope


def passing_at(level, wet, exponent):
    ratio = (level + 1).astype(F32) / EUPHOTIC
    ratio = jnp.maximum(ratio, 1.0)
    reaching = jnp.where(level >= EUPHOTIC - 1, jnp.exp(-1.5 * exponent * jnp.log(ratio)), 1.0)
    return jnp.where(level < wet - 1, reaching, 0.0)


def prepare_kernel(size, small, *refs):
    state_hbm, krylov_hbm = refs[:2]
    small_hbm = refs[2 : 2 + small]
    low_ref, high_ref, send_ref = refs[2 + small : 5 + small]
    small_refs = refs[5 + small : 5 + 2 * small]
    state_ref, krylov_ref, fields_ref, semaphore = refs[5 + 2 * small :]
    pairs = [(state_hbm, state_ref), (krylov_hbm, krylov_ref), *zip(small_hbm, small_refs)]
    copies = [
        pltpu.make_async_copy(source, target, semaphore.at[place])
        for place, (source, target) in enumerate(pairs)
    ]
    for copy in copies:
        copy.start()
    fields_ref[...] = jnp.zeros_like(fields_ref)
    copies[0].wait()
    copies[1].wait()
    for channel in range(CHANNELS):
        source = state_ref if channel < 2 else krylov_ref
        fields_ref[pl.ds(channel, size.levels, stride=CHANNELS), :] = source[:, channel % 2, :]
    low_ref[...] = fields_ref[: size.low_rows, :]
    high_ref[...] = fields_ref[size.low_rows : size.low_rows + size.high_rows, :]
    send_ref[...] = fields_ref[: size.send_rows, :].astype(BF16)
    for copy in copies[2:]:
        copy.wait()


def local_kernel(size, stage, *refs):
    low_ref, high_ref, wet_ref, light_ref = refs[:4]
    if stage == "first":
        exponent_ref, columns_ref, explicit_ref, implicit_ref = refs[4:8]
        partial_ref, next_high_ref, total_ref, remineral_ref, depth_ref = refs[8:13]
        fields_ref, middle_ref, rate_ref = refs[13:]
    else:
        remineral_ref, explicit_ref, implicit_ref = refs[4:7]
        if stage == "middle":
            total_in_ref, partial_ref, next_high_ref, total_ref = refs[7:11]
        else:
            partial_ref, next_high_ref = refs[7:9]
        fields_ref, middle_ref, rate_ref = refs[-3:]
    columns = size.columns
    wet = wet_ref[...]
    light = light_ref[...]
    zero_edge = jnp.zeros((EDGE, columns), F32)
    live = PAIR * size.pairs
    for ref in (fields_ref, middle_ref):
        ref[:EDGE, :] = zero_edge
        for start in range(EDGE + live, size.padded, PAIR):
            ref[start : start + PAIR, :] = zero_edge
    fields_ref[EDGE : EDGE + size.low_rows, :] = low_ref[...]
    fields_ref[EDGE + size.low_rows : EDGE + live, :] = high_ref[...]
    if stage == "first":
        exponent = exponent_ref[...]
        level = lax.broadcasted_iota(jnp.int32, (size.rows // CHANNELS, columns), 0)
        above = jnp.where(level == 0, 1.0, passing_at(level - 1, wet, exponent))
        share = time_step * (above - passing_at(level, wet, exponent))
        blank = jnp.zeros_like(share)
        for channel in range(CHANNELS):
            remineral_ref[pl.ds(channel, size.rows // CHANNELS, stride=CHANNELS), :] = (
                blank if channel % 2 else share
            )
        here = (columns_ref[...] != size.levels).astype(F32)
        depth = jnp.sum(here, axis=1, keepdims=True).astype(jnp.int32)
        depth_ref[...] = jnp.broadcast_to(depth, depth_ref.shape)
    uptake, slope = uptake_of(fields_ref, EDGE, wet, light, columns)
    export = (1.0 - dop_fraction) * jnp.sum(uptake, axis=0, keepdims=True)
    export_slope = (1.0 - dop_fraction) * jnp.sum(slope, axis=0, keepdims=True)
    if stage == "first":
        total_ref[...] = export
    elif stage == "middle":
        total_ref[...] = total_in_ref[...] + export
    for channel, rate in enumerate((uptake, uptake, slope, slope)):
        factor = time_step * (dop_fraction if channel % 2 else -1.0)
        rate_ref[pl.ds(channel, PAIR, stride=CHANNELS), :] = factor * rate
    row = sublane(columns)
    sinking = jnp.where(row % CHANNELS < 2, export, export_slope)
    organic_row = row % 2 == 1

    def sources(pair):
        top = PAIR * pair
        own = fields_ref[EDGE + top : EDGE + top + PAIR, :]
        following = fields_ref[EDGE + top + 1 : EDGE + top + PAIR + 1, :]
        decayed = (time_step * dop_decay) * jnp.where(organic_row, -own, following)
        rate = jnp.where(wet_rows(pair, wet, columns), decayed, 0.0)
        rate = rate + remineral_ref[top : top + PAIR, :] * sinking
        if top < CHANNELS * PAIR:
            rate = rate + rate_ref[top : top + PAIR, :]
        return rate

    for quad in range(size.quads):
        lhs = window(fields_ref, EDGE + QUAD * quad, (0, -CHANNELS, CHANNELS))
        for pair in range(2 * quad, min(2 * quad + 2, size.pairs)):
            top = PAIR * pair
            value = pair_product(lhs, explicit_ref, pair, columns) + sources(pair)
            partial_ref[top : top + PAIR, :] = value
            middle_ref[EDGE + top : EDGE + top + PAIR, :] = value
    for start in range(live, size.rows, PAIR):
        partial_ref[start : start + PAIR, :] = zero_edge
    for quad in range(size.low_pairs // 2, size.quads):
        lhs = window(middle_ref, EDGE + QUAD * quad, (-CHANNELS, 0, CHANNELS))
        for pair in range(max(2 * quad, size.low_pairs), min(2 * quad + 2, size.pairs)):
            settled = pair_product(lhs, implicit_ref, pair, columns)
            top = PAIR * (pair - size.low_pairs)
            next_high_ref[top : top + PAIR, :] = jnp.where(
                wet_rows(pair, wet, columns), settled, 0.0
            )


def place_slots(total, slots_ref, slots, width):
    targets = slots_ref.shape[0]
    column = lax.broadcasted_iota(jnp.int32, (targets, total.shape[1]), 1)
    lane = lax.broadcasted_iota(jnp.int32, (targets, width), 1) - slots * lax.axis_index("tile")
    placed = jnp.zeros((targets, width), F32)
    for slot in range(slots):
        chosen = column == slots_ref[:, slot : slot + 1]
        value = jnp.sum(jnp.where(chosen, total, 0.0), axis=1, keepdims=True)
        placed = jnp.where(lane == slot, value, placed)
    return placed


def halves(rows):
    half = rows.shape[0] // 2
    upper = (lax.axis_index("tile") // half) % 2 == 1
    first, second = rows[:half], rows[half:]
    return jnp.where(upper, second, first), jnp.where(upper, first, second)


def quarters(rows):
    mine, other = halves(rows)
    return (*halves(mine), *halves(other))


def pack(rows):
    high = rows.astype(BF16).astype(F32)
    return jnp.concatenate(
        [
            part[:, start : start + 128]
            for part in (high, rows - high)
            for start in range(0, rows.shape[1], 128)
        ],
        axis=0,
    )


def unpack(packed, count, width):
    blocks = width // 128
    parts = [packed[count * k : count * (k + 1)] for k in range(2 * blocks)]
    high = jnp.concatenate(parts[:blocks], axis=1)
    return high + jnp.concatenate(parts[blocks:], axis=1)


def route_kernel(arrivals, first, *refs):
    kept_ref, *arrived_refs = refs[: 1 + arrivals]
    out_refs = refs[1 + arrivals :]
    rows = kept_ref[...]
    count, width = rows.shape
    if first:
        packed = arrived_refs.pop()
        start = packed.shape[0] - 2 * count * (width // 128)
        rows = rows + unpack(packed[start:, :].astype(F32), count, width)
    for ref in arrived_refs:
        rows = rows + ref[...]
    for ref, part in zip(out_refs, quarters(rows) if len(out_refs) == 4 else halves(rows)):
        ref[...] = part


def flux_kernel(*refs):
    *part_refs, flux_ref = refs
    flux = part_refs[0][...]
    for ref in part_refs[1:]:
        flux = flux + ref[...]
    flux_ref[...] = flux[:, : flux_ref.shape[1]]


def ghost_kernel(size, stage, slots, *refs):
    partial_ref, pair_ref, other_ref, across_ref, depth_ref, wet_ref, explicit_ref, implicit_ref = refs[:8]
    if stage == "last":
        high_ref, state_ref, tangent_ref, middle_ref, fields_ref = refs[8:]
    elif stage == "export":
        light_ref, total_ref, slots_ref, low_ref, send_ref, across_out_ref = refs[8:14]
        keep_ref, near_ref, far_ref, middle_ref = refs[14:]
    else:
        low_ref, send_ref, middle_ref = refs[8:]
    columns = size.columns
    wet = wet_ref[...]
    even = lax.axis_index("tile") % 2 == 0
    middle_ref[:EDGE, :] = jnp.zeros((EDGE, columns), F32)
    for top in range(PAIR * size.ghost_pairs, QUAD * size.low_quads + EDGE, PAIR):
        middle_ref[EDGE + top : EDGE + top + PAIR, :] = partial_ref[top : top + PAIR, :]
    for quad in range(size.ghost_quads):
        span = slice(QUAD * quad, QUAD * quad + QUAD)
        own_chip = pair_ref[span, :].astype(F32)
        next_chip = other_ref[span, :].astype(F32)
        across = across_ref[span, :].astype(F32)
        level = lax.broadcasted_iota(jnp.int32, (QUAD, columns), 0) // CHANNELS + CHANNELS * quad
        before = jnp.where(even, next_chip, own_chip)
        after = jnp.where(even, own_chip, next_chip)
        before = jnp.where(level < depth_ref[3:4, :], before, 0.0)
        after = jnp.where(level < depth_ref[4:5, :], after, 0.0)
        across = jnp.where(level < depth_ref[5:6, :], across, 0.0)
        lhs = jnp.concatenate([before, after, across], axis=1).astype(BF16)
        for pair in range(2 * quad, min(2 * quad + 2, size.ghost_pairs)):
            top = PAIR * pair
            value = pair_product(lhs, explicit_ref, pair, columns, 3)
            middle_ref[EDGE + top : EDGE + top + PAIR, :] = value + partial_ref[top : top + PAIR, :]
    values = []
    for quad in range(size.low_quads):
        lhs = window(middle_ref, EDGE + QUAD * quad, (-CHANNELS, 0, CHANNELS))
        for pair in range(2 * quad, min(2 * quad + 2, size.low_pairs)):
            settled = pair_product(lhs, implicit_ref, pair, columns)
            values.append(jnp.where(wet_rows(pair, wet, columns), settled, 0.0))
    if stage == "last":
        for pair, value in enumerate(values):
            fields_ref[PAIR * pair : PAIR * pair + PAIR, :] = value
        fields_ref[size.low_rows : size.low_rows + size.high_rows, :] = high_ref[...]
        for channel in range(CHANNELS):
            out_ref = state_ref if channel < 2 else tangent_ref
            out_ref[:, channel % 2, :] = fields_ref[pl.ds(channel, size.levels, stride=CHANNELS), :]
        return
    for pair, value in enumerate(values):
        low_ref[PAIR * pair : PAIR * pair + PAIR, :] = value
    blank = jnp.zeros((PAIR, columns), F32)
    for quad in range(size.ghost_quads):
        two = [
            values[pair] if pair < len(values) else blank for pair in (2 * quad, 2 * quad + 1)
        ]
        rows = jnp.concatenate(two, axis=0).astype(BF16)
        send_ref[QUAD * quad : QUAD * quad + QUAD, :] = rows
        if stage == "export":
            across_out_ref[QUAD * quad : QUAD * quad + QUAD, :] = rows
    if stage == "export":
        uptake, _ = uptake_of(low_ref, 0, wet, light_ref[...], columns)
        total = total_ref[...] + (1.0 - dop_fraction) * jnp.sum(uptake, axis=0, keepdims=True)
        placed = place_slots(total, slots_ref, slots, keep_ref.shape[1])
        keep_ref[...], near_ref[...], leaving, far_ref[...] = quarters(placed)
        across_out_ref[size.send_rows :, :] = pack(leaving).astype(BF16)


def in_vmem(value):
    return pltpu.with_memory_space_constraint(value, pltpu.VMEM)


def call(body, outputs, scratch, operands, flops=1000000, in_hbm=()):
    space = lambda place: pltpu.HBM if place in in_hbm else pltpu.VMEM
    operands = [
        pltpu.with_memory_space_constraint(value, pltpu.HBM) if place in in_hbm else value
        for place, value in enumerate(operands)
    ]
    return pl.pallas_call(
        body,
        out_shape=outputs,
        in_specs=[pl.BlockSpec(memory_space=space(k)) for k in range(len(operands))],
        out_specs=[pl.BlockSpec(memory_space=pltpu.VMEM)] * len(outputs),
        scratch_shapes=scratch,
        compiler_params=pltpu.CompilerParams(vmem_limit_bytes=8 * MIB),
        cost_estimate=pl.CostEstimate(flops=flops, bytes_accessed=100000, transcendentals=0),
    )(*operands)


def on_device(
    tracer_state,
    krylov_direction,
    explicit_tiles,
    implicit_tiles,
    explicit_columns,
    ghost_levels,
    wet_levels,
    surface_light,
    martin_exponent,
    column_slots,
):
    size = Sizes(tracer_state.shape[1], tracer_state.shape[2], ghost_levels.shape[1])
    columns = size.columns
    tile_count = lax.axis_size("tile")
    assert tile_count & (tile_count - 1) == 0
    slots = column_slots.shape[1]
    width = -(-tile_count * slots // 128) * 128
    row_of = lambda value: value.reshape(1, columns)
    explicit, implicit = in_vmem(explicit_tiles), in_vmem(implicit_tiles)

    same_chip = [(d, d ^ 1) for d in range(tile_count)]
    next_chip = [(d, (d + (1 if d % 2 else -1)) % tile_count) for d in range(tile_count)]
    opposite = [(d, (d + tile_count // 2) % tile_count) for d in range(tile_count)]

    def exchange(value, across_value):
        across = lax.ppermute(across_value, "tile", opposite)
        other = lax.ppermute(value, "tile", next_chip)
        pair = lax.ppermute(value, "tile", same_chip)
        return pair, other, across

    def hop(value, away):
        partners = [(d, d ^ away) for d in range(tile_count)]
        return lax.ppermute(value, "tile", partners)

    def shape(rows, dtype=F32):
        return pltpu.VMEM((rows, columns), dtype)

    padded = pltpu.VMEM((size.padded, columns), F32)
    low_scratch = pltpu.VMEM((QUAD * size.low_quads + 2 * EDGE, columns), F32)
    local_scratch = [padded, padded, pltpu.VMEM((CHANNELS * PAIR, columns), F32)]
    depth_shape = pltpu.VMEM((explicit_columns.shape[1], columns), jnp.int32)

    small = [
        row_of(wet_levels),
        row_of(surface_light),
        row_of(martin_exponent),
        explicit_columns.T,
        column_slots,
    ]
    tall = pltpu.VMEM((size.levels, CHANNELS // 2, columns), F32)
    low, high, send, wet, light, exponent, column_rows, slot_rows = call(
        functools.partial(prepare_kernel, size, len(small)),
        [shape(size.low_rows), shape(size.high_rows), shape(size.send_rows, BF16)]
        + [pltpu.VMEM(value.shape, value.dtype) for value in small],
        [
            tall,
            tall,
            pltpu.VMEM((size.rows, columns), F32),
            pltpu.SemaphoreType.DMA((2 + len(small),)),
        ],
        [tracer_state.transpose(1, 0, 2), krylov_direction.transpose(1, 0, 2)] + small,
        PREPARE_FLOPS,
        tuple(range(2 + len(small))),
    )
    across_send = send
    for time_index in range(STEPS):
        first, last = time_index == 0, time_index == STEPS - 1
        ghosts = exchange(send, across_send)
        operands = [low, high, wet, light]
        outputs = [shape(size.rows), shape(size.high_rows)]
        weights = [explicit, implicit]
        if first:
            partial, high, total, remineral, depth = call(
                functools.partial(local_kernel, size, "first"),
                outputs + [shape(1), shape(size.rows), depth_shape],
                local_scratch,
                operands + [exponent, column_rows] + weights,
                4000000,
            )
        elif last:
            partial, high = call(
                functools.partial(local_kernel, size, "last"),
                outputs,
                local_scratch,
                operands + [remineral] + weights,
                4000000,
            )
        else:
            partial, high, total = call(
                functools.partial(local_kernel, size, "middle"),
                outputs + [shape(1)],
                local_scratch,
                operands + [remineral] + weights + [total],
                4000000,
            )
        operands = [partial, *ghosts, depth, wet] + weights
        sends = [shape(size.low_rows), shape(size.send_rows, BF16)]
        if last:
            result = jax.ShapeDtypeStruct((size.levels, CHANNELS // 2, columns), F32)
            state_out, tangent_out = call(
                functools.partial(ghost_kernel, size, "last", slots),
                [result, result],
                [low_scratch, pltpu.VMEM((size.rows, columns), F32)],
                operands + [high],
                2000000,
            )
        elif time_index == STEPS - 2:
            quarter = tile_count // 4
            packed_rows = size.send_rows + 2 * quarter * (width // 128)
            low, send, across_send, kept, near, far = call(
                functools.partial(ghost_kernel, size, "export", slots),
                sends + [shape(packed_rows, BF16)] + [pltpu.VMEM((quarter, width), F32)] * 3,
                [low_scratch],
                operands + [light, total, slot_rows],
            )
            hops = [hop(near, quarter), hop(far, 3 * quarter)]
        else:
            low, send = call(
                functools.partial(ghost_kernel, size, "middle", slots),
                sends,
                [low_scratch],
                operands,
            )
            across_send = send
    arrived, rest = [*hops, ghosts[2]], tile_count // 4
    while rest > 1:
        step = 4 if rest >= 4 else 2
        rest //= step
        kept, *leaving = call(
            functools.partial(route_kernel, len(arrived), 4 * step * rest == tile_count),
            [pltpu.VMEM((rest, width), F32)] * step,
            [],
            [kept, *arrived],
        )
        arrived = [hop(value, place * rest) for place, value in enumerate(leaving, 1)]
    (flux,) = call(
        flux_kernel, [jax.ShapeDtypeStruct((1, tile_count * slots), F32)], [], [kept, *arrived]
    )
    return state_out.transpose(1, 0, 2), tangent_out.transpose(1, 0, 2), flux.reshape(-1)


def solution(mesh):
    return jax.shard_map(
        on_device,
        mesh=mesh,
        in_specs=(
            P(None, None, ("groups", "tile")),
            P(None, None, ("groups", "tile")),
            P("tile", None, None, None),
            P("tile", None, None, None),
            P("tile", None),
            P("tile", None),
            P("tile"),
            P(("groups", "tile")),
            P(("groups", "tile")),
            P("tile", None),
        ),
        out_specs=(
            P(None, None, ("groups", "tile")),
            P(None, None, ("groups", "tile")),
            P(("groups", "tile")),
        ),
        check_vma=False,
    )
```

```python
import functools

import jax
import jax.numpy as jnp
from jax import lax
from jax.experimental import pallas as pl
from jax.experimental.pallas import tpu as pltpu
from jax.sharding import PartitionSpec as P


EUPHOTIC = 6
STEPS = 3

max_uptake = 1.0
half_saturation = 0.5
dop_fraction = 0.67
dop_decay = 0.2
time_step = 0.5

F32 = jnp.float32
BF16 = jnp.bfloat16
MIB = 1 << 20
PREPARE_FLOPS = 10**10

CHANNELS = 4
PAIR = 2 * CHANNELS
QUAD = 4 * CHANNELS
EDGE = PAIR


class Sizes:
    def __init__(self, levels, columns, depth):
        self.levels = levels
        self.columns = columns
        self.pairs = levels // 2
        self.quads = (levels + 3) // 4
        self.rows = QUAD * self.quads
        self.padded = self.rows + 2 * EDGE
        self.ghost_pairs = (depth + 1) // 2
        self.low_pairs = min((depth + 2) // 2, self.pairs)
        self.ghost_quads = (self.ghost_pairs + 1) // 2
        self.low_quads = (self.low_pairs + 1) // 2
        self.send_rows = QUAD * self.ghost_quads
        self.low_rows = PAIR * self.low_pairs
        self.high_rows = PAIR * (self.pairs - self.low_pairs)


def sublane(columns):
    return lax.broadcasted_iota(jnp.int32, (PAIR, columns), 0)


def own_halves(lhs, rhs, pair, columns):
    product = jnp.dot(lhs, rhs, preferred_element_type=F32)
    top = PAIR * (pair % 2)
    upper = product[top : top + PAIR, :columns]
    lower = product[top : top + PAIR, columns:]
    return jnp.where(sublane(columns) < CHANNELS, upper, lower)


def tiles_of(ref, level, first, columns):
    return ref[level, first : first + 3].reshape(3 * columns, columns)


def pair_product(lhs, ref, pair, columns, first=0):
    rhs = jnp.concatenate(
        [tiles_of(ref, 2 * pair, first, columns), tiles_of(ref, 2 * pair + 1, first, columns)],
        axis=1,
    )
    return own_halves(lhs, rhs, pair, columns)


def chosen_product(lhs, ref, pair, tiles, columns):
    blocks = [
        jnp.concatenate([ref[level, tile] for tile in tiles], axis=0)
        for level in (2 * pair, 2 * pair + 1)
    ]
    return own_halves(lhs, jnp.concatenate(blocks, axis=1), pair, columns)


def window(ref, start, offsets):
    parts = [ref[start + offset : start + offset + QUAD, :] for offset in offsets]
    return jnp.concatenate(parts, axis=1).astype(BF16)


def wet_rows(pair, wet, columns):
    return (2 * pair + sublane(columns) // CHANNELS) < wet


def uptake_of(ref, base, wet, light, columns):
    level = lax.broadcasted_iota(jnp.int32, (PAIR, columns), 0)
    phosphate = ref[pl.ds(base, PAIR, stride=CHANNELS), :]
    direction = ref[pl.ds(base + 2, PAIR, stride=CHANNELS), :]
    scale = max_uptake * light * jnp.exp(-2.0 * level.astype(F32) / EUPHOTIC)
    scale = jnp.where((level < EUPHOTIC) & (level < wet), scale, 0.0)
    squared = phosphate * phosphate
    half = half_saturation**2
    inverse = 1.0 / (half + squared)
    uptake = scale * squared * inverse
    slope = scale * half * (2.0 * phosphate * direction) * inverse * inverse
    return uptake, slope


def passing_at(level, wet, exponent):
    ratio = (level + 1).astype(F32) / EUPHOTIC
    ratio = jnp.maximum(ratio, 1.0)
    reaching = jnp.where(level >= EUPHOTIC - 1, jnp.exp(-1.5 * exponent * jnp.log(ratio)), 1.0)
    return jnp.where(level < wet - 1, reaching, 0.0)


def prepare_kernel(size, small, *refs):
    state_hbm, krylov_hbm = refs[:2]
    small_hbm = refs[2 : 2 + small]
    low_ref, high_ref, send_ref = refs[2 + small : 5 + small]
    small_refs = refs[5 + small : 5 + 2 * small]
    state_ref, krylov_ref, fields_ref, semaphore = refs[5 + 2 * small :]
    pairs = [(state_hbm, state_ref), (krylov_hbm, krylov_ref), *zip(small_hbm, small_refs)]
    copies = [
        pltpu.make_async_copy(source, target, semaphore.at[place])
        for place, (source, target) in enumerate(pairs)
    ]
    for copy in copies:
        copy.start()
    fields_ref[...] = jnp.zeros_like(fields_ref)
    copies[0].wait()
    copies[1].wait()
    for channel in range(CHANNELS):
        source = state_ref if channel < 2 else krylov_ref
        fields_ref[pl.ds(channel, size.levels, stride=CHANNELS), :] = source[:, channel % 2, :]
    low_ref[...] = fields_ref[: size.low_rows, :]
    high_ref[...] = fields_ref[size.low_rows : size.low_rows + size.high_rows, :]
    send_ref[...] = fields_ref[: size.send_rows, :].astype(BF16)
    for copy in copies[2:]:
        copy.wait()


def local_kernel(size, stage, *refs):
    low_ref, high_ref, wet_ref, light_ref = refs[:4]
    if stage == "first":
        exponent_ref, columns_ref, explicit_ref, implicit_ref = refs[4:8]
        partial_ref, next_high_ref, total_ref, remineral_ref, depth_ref = refs[8:13]
        fields_ref, middle_ref, rate_ref = refs[13:]
    else:
        remineral_ref, explicit_ref, implicit_ref = refs[4:7]
        if stage == "middle":
            total_in_ref, partial_ref, next_high_ref, total_ref = refs[7:11]
        else:
            partial_ref, next_high_ref = refs[7:9]
        fields_ref, middle_ref, rate_ref = refs[-3:]
    columns = size.columns
    wet = wet_ref[...]
    light = light_ref[...]
    zero_edge = jnp.zeros((EDGE, columns), F32)
    live = PAIR * size.pairs
    for ref in (fields_ref, middle_ref):
        ref[:EDGE, :] = zero_edge
        for start in range(EDGE + live, size.padded, PAIR):
            ref[start : start + PAIR, :] = zero_edge
    fields_ref[EDGE : EDGE + size.low_rows, :] = low_ref[...]
    fields_ref[EDGE + size.low_rows : EDGE + live, :] = high_ref[...]
    if stage == "first":
        exponent = exponent_ref[...]
        level = lax.broadcasted_iota(jnp.int32, (size.rows // CHANNELS, columns), 0)
        above = jnp.where(level == 0, 1.0, passing_at(level - 1, wet, exponent))
        share = time_step * (above - passing_at(level, wet, exponent))
        blank = jnp.zeros_like(share)
        for channel in range(CHANNELS):
            remineral_ref[pl.ds(channel, size.rows // CHANNELS, stride=CHANNELS), :] = (
                blank if channel % 2 else share
            )
        here = (columns_ref[...] != size.levels).astype(F32)
        depth = jnp.sum(here, axis=1, keepdims=True).astype(jnp.int32)
        depth_ref[...] = jnp.broadcast_to(depth, depth_ref.shape)
    uptake, slope = uptake_of(fields_ref, EDGE, wet, light, columns)
    export = (1.0 - dop_fraction) * jnp.sum(uptake, axis=0, keepdims=True)
    export_slope = (1.0 - dop_fraction) * jnp.sum(slope, axis=0, keepdims=True)
    if stage == "first":
        total_ref[...] = export
    elif stage == "middle":
        total_ref[...] = total_in_ref[...] + export
    for channel, rate in enumerate((uptake, uptake, slope, slope)):
        factor = time_step * (dop_fraction if channel % 2 else -1.0)
        rate_ref[pl.ds(channel, PAIR, stride=CHANNELS), :] = factor * rate
    row = sublane(columns)
    sinking = jnp.where(row % CHANNELS < 2, export, export_slope)
    organic_row = row % 2 == 1

    def sources(pair):
        top = PAIR * pair
        own = fields_ref[EDGE + top : EDGE + top + PAIR, :]
        following = fields_ref[EDGE + top + 1 : EDGE + top + PAIR + 1, :]
        decayed = (time_step * dop_decay) * jnp.where(organic_row, -own, following)
        rate = jnp.where(wet_rows(pair, wet, columns), decayed, 0.0)
        rate = rate + remineral_ref[top : top + PAIR, :] * sinking
        if top < CHANNELS * PAIR:
            rate = rate + rate_ref[top : top + PAIR, :]
        return rate

    for quad in range(size.quads):
        lhs = window(fields_ref, EDGE + QUAD * quad, (0, -CHANNELS, CHANNELS))
        for pair in range(2 * quad, min(2 * quad + 2, size.pairs)):
            top = PAIR * pair
            value = pair_product(lhs, explicit_ref, pair, columns) + sources(pair)
            partial_ref[top : top + PAIR, :] = value
            middle_ref[EDGE + top : EDGE + top + PAIR, :] = value
    for start in range(live, size.rows, PAIR):
        partial_ref[start : start + PAIR, :] = zero_edge
    for quad in range(size.low_pairs // 2, size.quads):
        lhs = window(middle_ref, EDGE + QUAD * quad, (-CHANNELS, 0, CHANNELS))
        for pair in range(max(2 * quad, size.low_pairs), min(2 * quad + 2, size.pairs)):
            settled = pair_product(lhs, implicit_ref, pair, columns)
            top = PAIR * (pair - size.low_pairs)
            next_high_ref[top : top + PAIR, :] = jnp.where(
                wet_rows(pair, wet, columns), settled, 0.0
            )


def place_slots(total, slots_ref, slots, width):
    targets = slots_ref.shape[0]
    column = lax.broadcasted_iota(jnp.int32, (targets, total.shape[1]), 1)
    lane = lax.broadcasted_iota(jnp.int32, (targets, width), 1) - slots * lax.axis_index("tile")
    placed = jnp.zeros((targets, width), F32)
    for slot in range(slots):
        chosen = column == slots_ref[:, slot : slot + 1]
        value = jnp.sum(jnp.where(chosen, total, 0.0), axis=1, keepdims=True)
        placed = jnp.where(lane == slot, value, placed)
    return placed


def halves(rows):
    half = rows.shape[0] // 2
    upper = (lax.axis_index("tile") // half) % 2 == 1
    first, second = rows[:half], rows[half:]
    return jnp.where(upper, second, first), jnp.where(upper, first, second)


def quarters(rows):
    mine, other = halves(rows)
    return (*halves(mine), *halves(other))


def pack(rows):
    high = rows.astype(BF16).astype(F32)
    return jnp.concatenate(
        [
            part[:, start : start + 128]
            for part in (high, rows - high)
            for start in range(0, rows.shape[1], 128)
        ],
        axis=0,
    )


def unpack(packed, count, width):
    blocks = width // 128
    parts = [packed[count * k : count * (k + 1)] for k in range(2 * blocks)]
    high = jnp.concatenate(parts[:blocks], axis=1)
    return high + jnp.concatenate(parts[blocks:], axis=1)


def route_kernel(arrivals, first, *refs):
    kept_ref, *arrived_refs = refs[: 1 + arrivals]
    out_refs = refs[1 + arrivals :]
    rows = kept_ref[...]
    count, width = rows.shape
    if first:
        packed = arrived_refs.pop()
        start = packed.shape[0] - 2 * count * (width // 128)
        rows = rows + unpack(packed[start:, :].astype(F32), count, width)
    for ref in arrived_refs:
        rows = rows + ref[...]
    for ref, part in zip(out_refs, quarters(rows) if len(out_refs) == 4 else halves(rows)):
        ref[...] = part


def finish_kernel(state_ref, tangent_ref, *refs):
    *part_refs, state_hbm, tangent_hbm, flux_hbm, flux_ref, semaphore = refs
    copies = [
        pltpu.make_async_copy(state_ref, state_hbm, semaphore.at[0]),
        pltpu.make_async_copy(tangent_ref, tangent_hbm, semaphore.at[1]),
    ]
    for copy in copies:
        copy.start()
    flux = part_refs[0][...]
    for ref in part_refs[1:]:
        flux = flux + ref[...]
    flux_ref[...] = flux[:, : flux_ref.shape[1]]
    copies.append(pltpu.make_async_copy(flux_ref, flux_hbm, semaphore.at[2]))
    copies[2].start()
    for copy in copies:
        copy.wait()


def ghost_level(quad, columns):
    return lax.broadcasted_iota(jnp.int32, (QUAD, columns), 0) // CHANNELS + CHANNELS * quad


def side_tile():
    return 3 + (lax.axis_index("tile") + 1) % 2


def early_kernel(size, partial_ref, pair_ref, across_ref, depth_ref, explicit_ref, out_ref):
    columns = size.columns
    side = side_tile()
    side_depth, across_depth = depth_ref[pl.ds(side, 1), :], depth_ref[5:6, :]
    for quad in range(size.ghost_quads):
        span = slice(QUAD * quad, QUAD * quad + QUAD)
        level = ghost_level(quad, columns)
        own_chip = jnp.where(level < side_depth, pair_ref[span, :].astype(F32), 0.0)
        across = jnp.where(level < across_depth, across_ref[span, :].astype(F32), 0.0)
        lhs = jnp.concatenate([own_chip, across], axis=1).astype(BF16)
        for pair in range(2 * quad, min(2 * quad + 2, size.ghost_pairs)):
            top = PAIR * pair
            value = chosen_product(lhs, explicit_ref, pair, (side, 5), columns)
            out_ref[top : top + PAIR, :] = value + partial_ref[top : top + PAIR, :]


def ghost_kernel(size, stage, slots, *refs):
    if stage == "last":
        partial_ref, pair_ref, other_ref, across_ref = refs[:4]
    else:
        partial_ref, early_ref, other_ref = refs[:3]
        refs = refs[:1] + refs
    depth_ref, wet_ref, explicit_ref, implicit_ref = refs[4:8]
    if stage == "last":
        high_ref, state_ref, tangent_ref, middle_ref, fields_ref = refs[8:]
    elif stage == "export":
        light_ref, total_ref, slots_ref, low_ref, send_ref, across_out_ref = refs[8:14]
        keep_ref, near_ref, far_ref, middle_ref = refs[14:]
    else:
        low_ref, send_ref, middle_ref = refs[8:]
    columns = size.columns
    wet = wet_ref[...]
    even = lax.axis_index("tile") % 2 == 0
    middle_ref[:EDGE, :] = jnp.zeros((EDGE, columns), F32)
    for top in range(PAIR * size.ghost_pairs, QUAD * size.low_quads + EDGE, PAIR):
        middle_ref[EDGE + top : EDGE + top + PAIR, :] = partial_ref[top : top + PAIR, :]
    next_tile = 7 - side_tile()
    for quad in range(size.ghost_quads):
        span = slice(QUAD * quad, QUAD * quad + QUAD)
        level = ghost_level(quad, columns)
        next_chip = other_ref[span, :].astype(F32)
        if stage == "last":
            own_chip = pair_ref[span, :].astype(F32)
            before = jnp.where(even, next_chip, own_chip)
            after = jnp.where(even, own_chip, next_chip)
            before = jnp.where(level < depth_ref[3:4, :], before, 0.0)
            after = jnp.where(level < depth_ref[4:5, :], after, 0.0)
            across = jnp.where(level < depth_ref[5:6, :], across_ref[span, :].astype(F32), 0.0)
            lhs = jnp.concatenate([before, after, across], axis=1).astype(BF16)
        else:
            next_depth = depth_ref[pl.ds(next_tile, 1), :]
            lhs = jnp.where(level < next_depth, next_chip, 0.0).astype(BF16)
        for pair in range(2 * quad, min(2 * quad + 2, size.ghost_pairs)):
            top = PAIR * pair
            if stage == "last":
                value = pair_product(lhs, explicit_ref, pair, columns, 3)
                value = value + partial_ref[top : top + PAIR, :]
            else:
                value = chosen_product(lhs, explicit_ref, pair, (next_tile,), columns)
                value = value + early_ref[top : top + PAIR, :]
            middle_ref[EDGE + top : EDGE + top + PAIR, :] = value
    values = []
    for quad in range(size.low_quads):
        lhs = window(middle_ref, EDGE + QUAD * quad, (-CHANNELS, 0, CHANNELS))
        for pair in range(2 * quad, min(2 * quad + 2, size.low_pairs)):
            settled = pair_product(lhs, implicit_ref, pair, columns)
            values.append(jnp.where(wet_rows(pair, wet, columns), settled, 0.0))
    if stage == "last":
        for pair, value in enumerate(values):
            fields_ref[PAIR * pair : PAIR * pair + PAIR, :] = value
        fields_ref[size.low_rows : size.low_rows + size.high_rows, :] = high_ref[...]
        for channel in range(CHANNELS):
            out_ref = state_ref if channel < 2 else tangent_ref
            out_ref[:, channel % 2, :] = fields_ref[pl.ds(channel, size.levels, stride=CHANNELS), :]
        return
    for pair, value in enumerate(values):
        low_ref[PAIR * pair : PAIR * pair + PAIR, :] = value
    blank = jnp.zeros((PAIR, columns), F32)
    for quad in range(size.ghost_quads):
        two = [
            values[pair] if pair < len(values) else blank for pair in (2 * quad, 2 * quad + 1)
        ]
        rows = jnp.concatenate(two, axis=0).astype(BF16)
        send_ref[QUAD * quad : QUAD * quad + QUAD, :] = rows
        if stage == "export":
            across_out_ref[QUAD * quad : QUAD * quad + QUAD, :] = rows
    if stage == "export":
        uptake, _ = uptake_of(low_ref, 0, wet, light_ref[...], columns)
        total = total_ref[...] + (1.0 - dop_fraction) * jnp.sum(uptake, axis=0, keepdims=True)
        placed = place_slots(total, slots_ref, slots, keep_ref.shape[1])
        keep_ref[...], near_ref[...], leaving, far_ref[...] = quarters(placed)
        across_out_ref[size.send_rows :, :] = pack(leaving).astype(BF16)


def in_vmem(value):
    return pltpu.with_memory_space_constraint(value, pltpu.VMEM)


def call(body, outputs, scratch, operands, flops=1000000, in_hbm=(), out_space=pltpu.VMEM):
    space = lambda place: pltpu.HBM if place in in_hbm else pltpu.VMEM
    operands = [
        pltpu.with_memory_space_constraint(value, pltpu.HBM) if place in in_hbm else value
        for place, value in enumerate(operands)
    ]
    return pl.pallas_call(
        body,
        out_shape=outputs,
        in_specs=[pl.BlockSpec(memory_space=space(k)) for k in range(len(operands))],
        out_specs=[pl.BlockSpec(memory_space=out_space)] * len(outputs),
        scratch_shapes=scratch,
        compiler_params=pltpu.CompilerParams(vmem_limit_bytes=8 * MIB),
        cost_estimate=pl.CostEstimate(flops=flops, bytes_accessed=100000, transcendentals=0),
    )(*operands)


def on_device(
    tracer_state,
    krylov_direction,
    explicit_tiles,
    implicit_tiles,
    explicit_columns,
    ghost_levels,
    wet_levels,
    surface_light,
    martin_exponent,
    column_slots,
):
    size = Sizes(tracer_state.shape[1], tracer_state.shape[2], ghost_levels.shape[1])
    columns = size.columns
    tile_count = lax.axis_size("tile")
    assert tile_count & (tile_count - 1) == 0
    slots = column_slots.shape[1]
    width = -(-tile_count * slots // 128) * 128
    row_of = lambda value: value.reshape(1, columns)
    explicit, implicit = in_vmem(explicit_tiles), in_vmem(implicit_tiles)

    same_chip = [(d, d ^ 1) for d in range(tile_count)]
    next_chip = [(d, (d + (1 if d % 2 else -1)) % tile_count) for d in range(tile_count)]
    opposite = [(d, (d + tile_count // 2) % tile_count) for d in range(tile_count)]

    def exchange(value, across_value):
        across = lax.ppermute(across_value, "tile", opposite)
        other = lax.ppermute(value, "tile", next_chip)
        pair = lax.ppermute(value, "tile", same_chip)
        return pair, other, across

    def hop(value, away):
        partners = [(d, d ^ away) for d in range(tile_count)]
        return lax.ppermute(value, "tile", partners)

    def shape(rows, dtype=F32):
        return pltpu.VMEM((rows, columns), dtype)

    padded = pltpu.VMEM((size.padded, columns), F32)
    low_scratch = pltpu.VMEM((QUAD * size.low_quads + 2 * EDGE, columns), F32)
    local_scratch = [padded, padded, pltpu.VMEM((CHANNELS * PAIR, columns), F32)]
    depth_shape = pltpu.VMEM((explicit_columns.shape[1], columns), jnp.int32)

    small = [
        row_of(wet_levels),
        row_of(surface_light),
        row_of(martin_exponent),
        explicit_columns.T,
        column_slots,
    ]
    tall = pltpu.VMEM((size.levels, CHANNELS // 2, columns), F32)
    low, high, send, wet, light, exponent, column_rows, slot_rows = call(
        functools.partial(prepare_kernel, size, len(small)),
        [shape(size.low_rows), shape(size.high_rows), shape(size.send_rows, BF16)]
        + [pltpu.VMEM(value.shape, value.dtype) for value in small],
        [
            tall,
            tall,
            pltpu.VMEM((size.rows, columns), F32),
            pltpu.SemaphoreType.DMA((2 + len(small),)),
        ],
        [tracer_state.transpose(1, 0, 2), krylov_direction.transpose(1, 0, 2)] + small,
        PREPARE_FLOPS,
        tuple(range(2 + len(small))),
    )
    across_send = send
    for time_index in range(STEPS):
        first, last = time_index == 0, time_index == STEPS - 1
        ghosts = exchange(send, across_send)
        operands = [low, high, wet, light]
        outputs = [shape(size.rows), shape(size.high_rows)]
        weights = [explicit, implicit]
        if first:
            partial, high, total, remineral, depth = call(
                functools.partial(local_kernel, size, "first"),
                outputs + [shape(1), shape(size.rows), depth_shape],
                local_scratch,
                operands + [exponent, column_rows] + weights,
                4000000,
            )
        elif last:
            partial, high = call(
                functools.partial(local_kernel, size, "last"),
                outputs,
                local_scratch,
                operands + [remineral] + weights,
                4000000,
            )
        else:
            partial, high, total = call(
                functools.partial(local_kernel, size, "middle"),
                outputs + [shape(1)],
                local_scratch,
                operands + [remineral] + weights + [total],
                4000000,
            )
        pair_ghost, other_ghost, across_ghost = ghosts
        if last:
            operands = [partial, *ghosts, depth, wet] + weights
        else:
            (early,) = call(
                functools.partial(early_kernel, size),
                [shape(PAIR * size.ghost_pairs)],
                [],
                [partial, pair_ghost, across_ghost, depth, explicit],
            )
            operands = [partial, early, other_ghost, depth, wet] + weights
        sends = [shape(size.low_rows), shape(size.send_rows, BF16)]
        if last:
            state_out, tangent_out = call(
                functools.partial(ghost_kernel, size, "last", slots),
                [tall, tall],
                [low_scratch, pltpu.VMEM((size.rows, columns), F32)],
                operands + [high],
                2000000,
            )
        elif time_index == STEPS - 2:
            quarter = tile_count // 4
            packed_rows = size.send_rows + 2 * quarter * (width // 128)
            low, send, across_send, kept, near, far = call(
                functools.partial(ghost_kernel, size, "export", slots),
                sends + [shape(packed_rows, BF16)] + [pltpu.VMEM((quarter, width), F32)] * 3,
                [low_scratch],
                operands + [light, total, slot_rows],
            )
            hops = [hop(near, quarter), hop(far, 3 * quarter)]
        else:
            low, send = call(
                functools.partial(ghost_kernel, size, "middle", slots),
                sends,
                [low_scratch],
                operands,
            )
            across_send = send
    arrived, rest = [*hops, ghosts[2]], tile_count // 4
    while rest > 1:
        step = 4 if rest >= 4 else 2
        rest //= step
        kept, *leaving = call(
            functools.partial(route_kernel, len(arrived), 4 * step * rest == tile_count),
            [pltpu.VMEM((rest, width), F32)] * step,
            [],
            [kept, *arrived],
        )
        arrived = [hop(value, place * rest) for place, value in enumerate(leaving, 1)]
    result = pltpu.HBM((size.levels, CHANNELS // 2, columns), F32)
    state_out, tangent_out, flux = call(
        finish_kernel,
        [result, result, pltpu.HBM((1, tile_count * slots), F32)],
        [pltpu.VMEM((1, tile_count * slots), F32), pltpu.SemaphoreType.DMA((3,))],
        [state_out, tangent_out, kept, *arrived],
        out_space=pltpu.HBM,
    )
    return state_out.transpose(1, 0, 2), tangent_out.transpose(1, 0, 2), flux.reshape(-1)


def solution(mesh):
    return jax.shard_map(
        on_device,
        mesh=mesh,
        in_specs=(
            P(None, None, ("groups", "tile")),
            P(None, None, ("groups", "tile")),
            P("tile", None, None, None),
            P("tile", None, None, None),
            P("tile", None),
            P("tile", None),
            P("tile"),
            P(("groups", "tile")),
            P(("groups", "tile")),
            P("tile", None),
        ),
        out_specs=(
            P(None, None, ("groups", "tile")),
            P(None, None, ("groups", "tile")),
            P(("groups", "tile")),
        ),
        check_vma=False,
    )
```
